8 devices in a mesh: side: 4 (over z, y, x), rep: 2 (over core).
Axes of the slice: x: 2, y: 2, z: 1, core: 2. Of those that a mesh axis runs over, the one named last changes fastest.
Arguments:
- w_up: float32 [4, 12, 960, 1280], P('side', None, 'rep')
- w_down: float32 [4, 12, 1280, 960], P('side', None, None, 'rep')
- g_up: float32 [4, 12, 960, 1280], P('side', None, 'rep')
- g_down: float32 [4, 12, 1280, 960], P('side', None, None, 'rep')
- learn_rate: float32 [], replicated
- prompts: bfloat16 [4, 8192, 480], P('side', 'rep')
- prompt_lens: int32 [2], P('rep')
Outputs:
- output 1: float32 [4, 12, 960, 1280], P('side', None, 'rep')
- output 2: float32 [4, 12, 1280, 960], P('side', None, None, 'rep')
- output 3: bfloat16 [4, 8192, 480], P('side', 'rep')
All inputs are finite; a program needn't handle non-finite values.
Results may differ from the reference program's by a relative error of at most 0.02.
Values are sent between devices in bfloat16 or wider.
A program may use at most 1 GiB of HBM per device.

```python
import jax
import jax.numpy as jnp
from jax import lax

SIDE_DEVS = 4
REP_DEVS = 2
MODEL_DIM = 960
FFN_DIM = 2560
LAYERS = 12
TOKENS = 4096
TP_WAYS = SIDE_DEVS // 2
FF_PIECE = FFN_DIM // TP_WAYS
D_PIECE = MODEL_DIM // TP_WAYS


def draw_lens(len_key):
    key_a, key_b = jax.random.split(len_key)
    low_len = max(1, TOKENS // 32)
    base_lens = jax.random.randint(key_a, (REP_DEVS,), low_len, TOKENS + 1, jnp.int32)
    full_slot = jax.random.randint(key_b, (), 0, REP_DEVS, jnp.int32)
    return jnp.where(jnp.arange(REP_DEVS) == full_slot, TOKENS, base_lens).astype(jnp.int32)


def setup_inputs(seed: int = 0) -> dict:
    sub_keys = jax.random.split(jax.random.key(seed), 7)
    up_shape = (TP_WAYS, LAYERS, MODEL_DIM, FF_PIECE)
    down_shape = (TP_WAYS, LAYERS, FF_PIECE, MODEL_DIM)
    up_scale = MODEL_DIM ** -0.5
    down_scale = 0.7 * FFN_DIM ** -0.5
    w_up = jax.random.normal(sub_keys[0], up_shape, jnp.float32) * up_scale
    w_down = jax.random.normal(sub_keys[1], down_shape, jnp.float32) * down_scale
    g_up = jax.random.normal(sub_keys[2], up_shape, jnp.float32) * up_scale
    g_down = jax.random.normal(sub_keys[3], down_shape, jnp.float32) * down_scale
    learn_rate = jax.random.uniform(sub_keys[4], (), jnp.float32, 0.02, 0.25)
    gen_rows = jax.random.normal(sub_keys[5], (TP_WAYS, REP_DEVS * TOKENS, D_PIECE), jnp.float32)
    prompts = jnp.concatenate([jnp.zeros_like(gen_rows), gen_rows], axis=0).astype(jnp.bfloat16)
    return {
        "w_up": jnp.concatenate([w_up, jnp.zeros_like(w_up)], axis=0),
        "w_down": jnp.concatenate([w_down, jnp.zeros_like(w_down)], axis=0),
        "g_up": jnp.concatenate([g_up, jnp.zeros_like(g_up)], axis=0),
        "g_down": jnp.concatenate([g_down, jnp.zeros_like(g_down)], axis=0),
        "learn_rate": learn_rate,
        "prompts": prompts,
        "prompt_lens": draw_lens(sub_keys[6]),
    }


def reference(w_up, w_down, g_up, g_down, learn_rate, prompts, prompt_lens):
    new_up = w_up - learn_rate * g_up
    new_down = w_down - learn_rate * g_down
    up_bf = new_up[:TP_WAYS].astype(jnp.bfloat16)
    down_bf = new_down[:TP_WAYS].astype(jnp.bfloat16)
    up_full = jnp.transpose(up_bf, (1, 2, 0, 3)).reshape(LAYERS, MODEL_DIM, FFN_DIM)
    down_full = jnp.transpose(down_bf, (1, 0, 2, 3)).reshape(LAYERS, FFN_DIM, MODEL_DIM)
    x_full = jnp.transpose(prompts[TP_WAYS:], (1, 0, 2)).reshape(REP_DEVS, TOKENS, MODEL_DIM)

    def layer_step(h_rows, layer_w):
        up_layer, down_layer = layer_w
        pre_act = jnp.dot(h_rows, up_layer, preferred_element_type=jnp.float32)
        act_bf = jax.nn.gelu(pre_act, approximate=True).astype(jnp.bfloat16)
        part_sum = jnp.dot(act_bf, down_layer, preferred_element_type=jnp.float32)
        return (h_rows.astype(jnp.float32) + part_sum).astype(jnp.bfloat16), None

    def one_replica(replica_in):
        row_block, length = replica_in
        h_rows, _ = lax.scan(layer_step, row_block, (up_full, down_full))
        keep_mask = jnp.arange(TOKENS)[:, None] < length
        return jnp.where(keep_mask, h_rows, jnp.zeros_like(h_rows))

    y_full = lax.map(one_replica, (x_full, prompt_lens))
    y_gen = jnp.transpose(y_full.reshape(REP_DEVS * TOKENS, TP_WAYS, D_PIECE), (1, 0, 2))
    outputs = jnp.concatenate([jnp.zeros_like(y_gen), y_gen], axis=0)
    return new_up, new_down, outputs
```

```python
import jax
import jax.numpy as jnp
from jax import lax
from jax.experimental import pallas as pl
from jax.experimental.pallas import tpu as pltpu
from jax.sharding import PartitionSpec as P


LATE_SHARE = 1
DIRECT_DOWN = 2
TILE = 256
ROW_RUN = 128
CHUNKS = (256, 256, 256, 256, 256)
LAST = (((1,), (1,)), ((), ()))
GELU_A = 0.7978845608
GELU_B = 0.7978845608 * 0.044715


def update_kernel(gen_ref, lr_ref, wu, gu, wd, gd, *refs):
    nu, nd, ub, db = refs[-4:]
    is_gen = gen_ref[0] == 1
    lr = lr_ref[0]

    @pl.when(is_gen)
    def _():
        nu[...] = jnp.zeros_like(nu)
        nd[...] = jnp.zeros_like(nd)

    @pl.when(jnp.logical_not(is_gen))
    def _():
        u = wu[...] - lr * gu[...]
        nu[...] = u
        ub[...] = u[0].astype(jnp.bfloat16)
        d = wd[...] - lr * gd[...]
        nd[...] = d
        db[...] = d[0].astype(jnp.bfloat16)


def update_group(gen, lr, w_up, g_up, w_down, g_down, prev, first, count):
    _, _, du, hp = w_up.shape
    split = 2
    ur = du // split

    def in_map(l, s, gen_ref, lr_ref):
        live = 1 - gen_ref[0]
        return (0, (first + l) * live, s * live, 0)

    def out_map(l, s, gen_ref, lr_ref):
        return (0, first + l, s, 0)

    def bf_map(l, s, gen_ref, lr_ref):
        return (l, s, 0)

    in_specs = [
        pl.BlockSpec((1, 1, ur, hp), in_map),
        pl.BlockSpec((1, 1, ur, hp), in_map),
        pl.BlockSpec((1, 1, ur, hp), in_map),
        pl.BlockSpec((1, 1, ur, hp), in_map),
    ]
    args = [w_up, g_up, w_down, g_down]
    aliases = {}
    if prev is not None:
        in_specs += [pl.BlockSpec(memory_space=pl.ANY)] * 2
        args += list(prev)
        aliases = {6: 0, 7: 1}
    nbytes = count * 2 * du * hp * 14
    return pl.pallas_call(
        update_kernel,
        grid_spec=pltpu.PrefetchScalarGridSpec(
            num_scalar_prefetch=2,
            grid=(count, split),
            in_specs=in_specs,
            out_specs=[
                pl.BlockSpec((1, 1, ur, hp), out_map),
                pl.BlockSpec((1, 1, ur, hp), out_map),
                pl.BlockSpec((1, ur, hp), bf_map),
                pl.BlockSpec((1, ur, hp), bf_map),
            ],
        ),
        out_shape=[
            jax.ShapeDtypeStruct(w_up.shape, jnp.float32),
            jax.ShapeDtypeStruct(w_down.shape, jnp.float32),
            jax.ShapeDtypeStruct((count, du, hp), jnp.bfloat16),
            jax.ShapeDtypeStruct((count, du, hp), jnp.bfloat16),
        ],
        input_output_aliases=aliases,
        cost_estimate=pl.CostEstimate(flops=nbytes * 30, bytes_accessed=nbytes, transcendentals=0),
        name="update",
    )(gen, lr, *args)


def gelu(z):
    t = jnp.tanh(z * (GELU_A + GELU_B * (z * z)))
    h = 0.5 * z
    return h + h * t


def mlp_kernel(live_ref, x_ref, *refs):
    ups, downs, out = refs[0:4], refs[4:8], refs[8]

    @pl.when(live_ref[pl.program_id(0)] == 1)
    def _():
        x0, x1 = x_ref[0], x_ref[1]
        acc0 = acc1 = None
        for q in range(2):
            at = 0
            for width in CHUNKS:
                cols = pl.ds(at, width)
                z = jnp.dot(x0, ups[2 * q][0, :, cols], preferred_element_type=jnp.float32)
                z = z + jnp.dot(x1, ups[2 * q + 1][0, :, cols], preferred_element_type=jnp.float32)
                u = gelu(z).astype(jnp.bfloat16)
                p0 = lax.dot_general(u, downs[2 * q][0, :, cols], LAST, preferred_element_type=jnp.float32)
                p1 = lax.dot_general(u, downs[2 * q + 1][0, :, cols], LAST, preferred_element_type=jnp.float32)
                acc0 = p0 if acc0 is None else acc0 + p0
                acc1 = p1 if acc1 is None else acc1 + p1
                at += width
        out[0] = (x0.astype(jnp.float32) + acc0).astype(jnp.bfloat16)
        out[1] = (x1.astype(jnp.float32) + acc1).astype(jnp.bfloat16)


def mlp_layer(live, act, ups, downs):
    _, rows, half = act.shape
    hp = ups[0][0].shape[2]

    def weight_spec(shape, place):
        return pl.BlockSpec((1,) + shape, lambda i, live_ref: (place, 0, 0), pipeline_mode=pl.Buffered(1))

    specs = [pl.BlockSpec((2, TILE, half), lambda i, live_ref: (0, i, 0))]
    specs += [weight_spec((half, hp), place) for _, place in ups]
    specs += [weight_spec((half, hp), place) for _, place in downs]
    flops = rows * 2 * half * 2 * hp * 4
    return pl.pallas_call(
        mlp_kernel,
        grid_spec=pltpu.PrefetchScalarGridSpec(
            num_scalar_prefetch=1,
            grid=(rows // TILE,),
            in_specs=specs,
            out_specs=pl.BlockSpec((2, TILE, half), lambda i, live_ref: (0, i, 0)),
        ),
        out_shape=jax.ShapeDtypeStruct(act.shape, jnp.bfloat16),
        compiler_params=pltpu.CompilerParams(vmem_limit_bytes=56 * 1024 * 1024),
        cost_estimate=pl.CostEstimate(flops=flops, bytes_accessed=24 * 1024 * 1024, transcendentals=rows * 2 * hp),
    )(live, act, *[a for a, _ in ups], *[a for a, _ in downs])


def solution(mesh):
    reps = mesh.shape["rep"]
    axes = ("side", "rep")

    def at(side, rep):
        return side * reps + rep

    pairs = [(t, c) for t in range(2) for c in range(2)]
    trade = [(at(t, c), at(1 - t, c)) for t, c in pairs]
    to_gen = [(at(t, c), at(2 + t, c)) for t, c in pairs]
    gen_trade = [(at(2 + t, c), at(3 - t, c)) for t, c in pairs]
    to_train = [(at(2 + t, c), at(t, c)) for t, c in pairs]
    core_swap = [(at(t, c), at(t, 1 - c)) for t, c in pairs]

    up_spec = P("side", None, "rep", None)
    down_spec = P("side", None, None, "rep")
    act_spec = P("side", "rep", None)

    def device_step(w_up, w_down, g_up, g_down, learn_rate, prompts, prompt_lens):
        side = lax.axis_index("side")
        core = lax.axis_index("rep")
        is_gen = side >= 2
        t = lax.rem(side, 2)
        tokens, half = prompts.shape[1], prompts.shape[2]
        part = tokens // 4

        gen = is_gen.astype(jnp.int32).reshape(1)
        lr = learn_rate.reshape(1)
        other_len = lax.ppermute(prompt_lens, "rep", [(0, 1), (1, 0)])

        def send(x, pairs):
            return lax.ppermute(x, axes, pairs)

        def after(x, *gates):
            gates = [g for g in gates if g is not None]
            return lax.optimization_barrier((x, *gates))[0] if gates else x

        w_down, g_down = jnp.swapaxes(w_down, 2, 3), jnp.swapaxes(g_down, 2, 3)
        layers = w_up.shape[1]

        prev = None
        own = []
        for layer in range(layers):
            new_up, new_down, ub, db = update_group(gen, lr, w_up, g_up, w_down, g_down, prev, layer, 1)
            prev = (new_up, new_down)
            own.append((ub, db))

        runs = jnp.swapaxes(prompts[0], 0, 1).reshape(half, part // ROW_RUN, 4, ROW_RUN)
        got = {}
        for dt in range(2):
            for dc in range(2):
                j = 2 * jnp.bitwise_xor(t, dt) + jnp.bitwise_xor(core, dc)
                mine = lax.dynamic_slice_in_dim(runs, j, 1, axis=2).reshape(half, part)
                perm = [(at(2 + a, b), at(a ^ dt, b ^ dc)) for a, b in pairs]
                got[dt, dc] = send(mine, perm)

        first = []
        for layer, (ub, db) in enumerate(own):
            ru = send(ub, trade)
            rd = send(db, trade if layer < DIRECT_DOWN else to_gen)
            first.append((ru, rd))
        own_p = [(send(ub, core_swap), send(db, core_swap)) for ub, db in own]

        swap = jnp.bitwise_xor(t, core) == 1
        near = jnp.concatenate([got[0, 0], got[0, 1]], axis=1)
        far = jnp.concatenate([got[1, 0], got[1, 1]], axis=1)
        act = jnp.swapaxes(jnp.stack([jnp.where(swap, far, near), jnp.where(swap, near, far)]), 1, 2)

        tiles = part // TILE
        first_row = jnp.arange(tiles) * (4 * TILE) + (2 * t + core) * ROW_RUN
        live = jnp.concatenate([first_row < prompt_lens[0], first_row < other_len[0]])
        live = (live & jnp.logical_not(is_gen)).astype(jnp.int32)

        second, last, recv, recv_p = {}, {}, {}, {}

        def second_hop(layer, act):
            if DIRECT_DOWN <= layer < layers:
                second[layer] = send(after(first[layer][1], act), gen_trade)

        def last_hop(layer, act):
            if DIRECT_DOWN <= layer < layers:
                last[layer] = send(after(second[layer], act), to_train)

        def share(layer, act):
            if layer >= layers:
                return
            ru, rd = first[layer]
            if layer >= DIRECT_DOWN:
                rd = last[layer]
            hops = (second.get(layer + 1), first[layer + 2][1] if layer + 2 < layers else None)
            ru, rd = after(ru, act), after(rd, act, *hops)
            recv[layer] = (ru, rd)
            recv_p[layer] = (send(ru, core_swap), send(rd, core_swap))

        for layer in range(layers):
            if layer == 0:
                for early in range(3):
                    second_hop(early, None)
                for early in range(2):
                    last_hop(early, None)
                share(0, None)
            gate = act if layer else None
            second_hop(layer + 3, gate)
            last_hop(layer + 2, gate)
            if layer + 1 < layers - LATE_SHARE:
                share(layer + 1, gate)
            elif layer not in recv:
                share(layer, gate)
            ups = [(w[layer][0], 0) for w in (own, own_p, recv, recv_p)]
            downs = [(w[layer][1], 0) for w in (own, own_p, recv, recv_p)]
            act = mlp_layer(live, act, ups, downs)

        act = jnp.swapaxes(act, 1, 2)
        back = {}
        for dt in range(2):
            halves = (act[0], act[1]) if dt == 0 else (act[1], act[0])
            cols = jnp.where(swap, halves[1], halves[0])
            for dc in range(2):
                perm = [(at(a, b), at(2 + (a ^ dt), b ^ dc)) for a, b in pairs]
                back[dt, dc] = lax.ppermute(cols[:, dc * part : (dc + 1) * part], axes, perm)
        by_core = {}
        for dt in range(2):
            lo, hi = back[dt, 0], back[dt, 1]
            by_core[dt] = [jnp.where(core == 0, lo, hi), jnp.where(core == 0, hi, lo)]
        ordered = [jnp.where(t == 0, by_core[0][c], by_core[1][c]) for c in range(2)]
        ordered += [jnp.where(t == 0, by_core[1][c], by_core[0][c]) for c in range(2)]
        y = jnp.stack([o.reshape(half, part // ROW_RUN, ROW_RUN) for o in ordered], axis=2)
        y = y.reshape(half, tokens)
        keep = (jnp.arange(tokens)[None, :] < prompt_lens[0]) & is_gen
        y = jnp.swapaxes(jnp.where(keep, y, jnp.zeros_like(y)), 0, 1)
        return prev[0], jnp.swapaxes(prev[1], 2, 3), y[None]

    return jax.shard_map(
        device_step,
        mesh=mesh,
        in_specs=(up_spec, down_spec, up_spec, down_spec, P(), act_spec, P("rep")),
        out_specs=(up_spec, down_spec, act_spec),
        check_vma=False,
    )
```

```python
import jax
import jax.numpy as jnp
from jax import lax
from jax.experimental import pallas as pl
from jax.experimental.pallas import tpu as pltpu
from jax.sharding import PartitionSpec as P


DIRECT = 2
TILE = 256
CHUNK = 256
UPDATE_SPLIT = 2
LAST = (((1,), (1,)), ((), ()))
GELU_A = 0.7978845608
GELU_B = 0.7978845608 * 0.044715
MESH = pl.DeviceIdType.MESH


def gelu(z):
    t = jnp.tanh(z * (GELU_A + GELU_B * (z * z)))
    h = 0.5 * z
    return h + h * t


def flip(index, by):
    return 1 - index if by else index


def stack_kernel(lr_ref, wu, gu, wd, gd, xt, *refs):
    outs, (own, recv, pown, pfwd), refs = refs[:4], refs[4:8], refs[8:]
    wv, act, xr, fbuf, obuf = refs[:5]
    s_own, r_own, s_main, r_main, s_fwd, r_fwd, s_b, r_b, s_c, s_x, r_x, sem_in, sem_out, sem_ld, sem_y = refs[5:]
    side, core = lax.axis_index("side"), lax.axis_index("rep")
    t = lax.rem(side, 2)
    layers, half, hidden = wu.shape
    rows = half // UPDATE_SPLIT
    part = xt.shape[1] // 4
    tiles = 2 * part // TILE

    def remote(src, dst, send, recv_sem, to):
        return pltpu.make_async_remote_copy(
            src_ref=src, dst_ref=dst, send_sem=send, recv_sem=recv_sem, device_id=to, device_id_type=MESH
        )

    def x_copy(dt, dc):
        slot = 2 * dt + dc
        to = (flip(t, dt), flip(core, dc))
        lane = pl.multiple_of((2 * to[0] + to[1]) * part, 128)
        return remote(xt.at[:, pl.ds(lane, part)], xr.at[slot], s_x.at[slot], r_x.at[slot], to)

    def own_copy(l, k):
        return remote(own.at[l, k], pown.at[l, k], s_own.at[l, k], r_own.at[l, k], (t, 1 - core))

    def main_copy(l, k, to_side):
        return remote(own.at[l, k], recv.at[l, k], s_main.at[l, k], r_main.at[l, k], (to_side, core))

    def fwd_copy(l, k):
        return remote(recv.at[l, k], pfwd.at[l, k], s_fwd.at[l, k], r_fwd.at[l, k], (t, 1 - core))

    def b_copy(l):
        return remote(recv.at[l, 1], recv.at[l, 0], s_b.at[l], r_b.at[l], (3 - t, core))

    def c_copy(l):
        return remote(recv.at[l, 0], recv.at[l, 1], s_c.at[l], r_main.at[l, 1], (t, core))

    @pl.when(side >= 2)
    def _():
        for dt in range(2):
            for dc in range(2):
                x_copy(dt, dc).start()

        def hop(l, carry):
            main_copy(l, 1, t).wait_recv()
            b_copy(l).start()

            @pl.when(l > DIRECT)
            def _():
                b_copy(l - 1).wait_recv()
                c_copy(l - 1).start()

            return carry

        lax.fori_loop(DIRECT, layers, hop, 0)
        b_copy(layers - 1).wait_recv()
        c_copy(layers - 1).start()

        def drain(l, carry):
            b_copy(l).wait_send()
            c_copy(l).wait_send()
            return carry

        lax.fori_loop(DIRECT, layers, drain, 0)
        for dt in range(2):
            for dc in range(2):
                x_copy(dt, dc).wait_send()

    @pl.when(side < 2)
    def _():
        lr = lr_ref[0]

        def loads(l, unit):
            k, h = unit // 2, unit % 2
            w, g = ((wu, gu), (wd, gd))[k]
            span = pl.ds(h * rows, rows)
            return (
                pltpu.make_async_copy(w.at[l, span], fbuf.at[h, 0], sem_in.at[h, 0]),
                pltpu.make_async_copy(g.at[l, span], fbuf.at[h, 1], sem_in.at[h, 1]),
            )

        def store(l, unit):
            k, h = unit // 2, unit % 2
            return pltpu.make_async_copy(obuf.at[h], own.at[l, k, pl.ds(h * rows, rows)], sem_out.at[h])

        def send(l, k):
            own_copy(l, k).start()
            if k == 0:
                main_copy(l, 0, 1 - t).start()
                return

            @pl.when(l < DIRECT)
            def _():
                main_copy(l, 1, 1 - t).start()

            @pl.when(l >= DIRECT)
            def _():
                main_copy(l, 1, 2 + t).start()

        for copy in loads(0, 0):
            copy.start()

        def update(l, carry):
            for unit in range(4):
                h = unit % 2
                if unit < 3:
                    for copy in loads(l, unit + 1):
                        copy.start()
                else:

                    @pl.when(l + 1 < layers)
                    def _():
                        for copy in loads(l + 1, 0):
                            copy.start()

                for copy in loads(l, unit):
                    copy.wait()
                if unit >= 2:
                    store(l, unit - 2).wait()
                    if h == 1:
                        send(l, 0)
                else:

                    @pl.when(l > 0)
                    def _():
                        store(l - 1, unit + 2).wait()
                        if h == 1:
                            send(l - 1, 1)

                obuf[h] = (fbuf[h, 0] - lr * fbuf[h, 1]).astype(jnp.bfloat16)
                store(l, unit).start()
            return carry

        lax.fori_loop(0, layers, update, 0)
        store(layers - 1, 2).wait()
        store(layers - 1, 3).wait()
        send(layers - 1, 1)

        for dt in range(2):
            for dc in range(2):
                x_copy(dt, dc).wait_recv()
        twist = lax.rem(core + t, 2)

        def x_in(step, carry):
            lane = pl.multiple_of(step * 128, 128)
            for dt in range(2):
                s = flip(twist, dt)
                for dc in range(2):
                    row = pl.multiple_of(dc * part + step * 128, 128)
                    act[s, pl.ds(row, 128), :] = jnp.transpose(xr[2 * dt + dc, :, pl.ds(lane, 128)])
            return carry

        lax.fori_loop(0, part // 128, x_in, 0)

        def fetch(l, k, place):
            src = (own, pown, recv, pfwd)[place]
            slot = lax.rem(l, 2)
            return pltpu.make_async_copy(src.at[l, k], wv.at[slot, k, place], sem_ld.at[k, place])

        def fetch_own(l):
            for k in range(2):
                fetch(l, k, 0).start()
                own_copy(l, k).wait_recv()
                fetch(l, k, 1).start()

        def fetch_recv(l):
            for k in range(2):
                main_copy(l, k, 1 - t).wait_recv()
                fwd_copy(l, k).start()
                fetch(l, k, 2).start()

        def fetch_fwd(l):
            for k in range(2):
                fwd_copy(l, k).wait_recv()
                fetch(l, k, 3).start()

        def fetched(l):
            for k in range(2):
                for place in range(4):
                    fetch(l, k, place).wait()

        fetch_own(0)
        fetch_recv(0)
        fetch_fwd(0)

        def step(index, carry):
            l, tile = index // tiles, index % tiles
            slot = lax.rem(l, 2)

            @pl.when(tile == 0)
            def _():
                @pl.when(l == layers - 1)
                def _():
                    fetch_recv(layers - 1)
                    fetch_fwd(layers - 1)

                fetched(l)

                @pl.when(l + 1 < layers)
                def _():
                    fetch_own(l + 1)

                @pl.when(l + 1 < layers - 1)
                def _():
                    fetch_recv(l + 1)

            @pl.when((tile == tiles // 2) & (l + 1 < layers - 1))
            def _():
                fetch_fwd(l + 1)

            span = pl.ds(pl.multiple_of(tile * TILE, TILE), TILE)
            x0, x1 = act[0, span, :], act[1, span, :]
            acc0 = acc1 = None
            for q in range(2):
                for at in range(0, hidden, CHUNK):
                    cols = pl.ds(at, CHUNK)
                    z = jnp.dot(x0, wv[slot, 0, 2 * q, :, cols], preferred_element_type=jnp.float32)
                    z = z + jnp.dot(x1, wv[slot, 0, 2 * q + 1, :, cols], preferred_element_type=jnp.float32)
                    u = gelu(z).astype(jnp.bfloat16)
                    p0 = lax.dot_general(u, wv[slot, 1, 2 * q, :, cols], LAST, preferred_element_type=jnp.float32)
                    p1 = lax.dot_general(u, wv[slot, 1, 2 * q + 1, :, cols], LAST, preferred_element_type=jnp.float32)
                    acc0 = p0 if acc0 is None else acc0 + p0
                    acc1 = p1 if acc1 is None else acc1 + p1
            act[0, span, :] = (x0.astype(jnp.float32) + acc0).astype(jnp.bfloat16)
            act[1, span, :] = (x1.astype(jnp.float32) + acc1).astype(jnp.bfloat16)
            return carry

        lax.fori_loop(0, layers * tiles, step, 0)

        def x_out(step, carry):
            lane = pl.multiple_of(step * 128, 128)
            for dt in range(2):
                s = flip(twist, dt)
                for dc in range(2):
                    row = pl.multiple_of(dc * part + step * 128, 128)
                    xr[2 * dt + dc, :, pl.ds(lane, 128)] = jnp.transpose(act[s, pl.ds(row, 128), :])
            return carry

        lax.fori_loop(0, part // 128, x_out, 0)
        y_copies = [pltpu.make_async_copy(xr.at[i], outs[i], sem_y.at[i]) for i in range(4)]
        for copy in y_copies:
            copy.start()
        for copy in y_copies:
            copy.wait()

        def drain(l, carry):
            for k in range(2):
                own_copy(l, k).wait_send()
                main_copy(l, k, 1 - t).wait_send()
                fwd_copy(l, k).wait_send()
            return carry

        lax.fori_loop(0, layers, drain, 0)


def mlp_stack(lr, w_up, g_up, w_down, g_down, xt):
    layers, half, hidden = w_up.shape
    part = xt.shape[1] // 4
    rows = half // UPDATE_SPLIT
    dma = pltpu.SemaphoreType.DMA
    any_spec = pl.BlockSpec(memory_space=pl.ANY)
    store = jax.ShapeDtypeStruct((layers, 2, half, hidden), jnp.bfloat16)
    return pl.pallas_call(
        stack_kernel,
        in_specs=[pl.BlockSpec(memory_space=pltpu.SMEM)] + [any_spec] * 5,
        out_specs=[any_spec] * 8,
        out_shape=[jax.ShapeDtypeStruct((half, part), jnp.bfloat16)] * 4 + [store] * 4,
        scratch_shapes=[
            pltpu.VMEM((2, 2, 4, half, hidden), jnp.bfloat16),
            pltpu.VMEM((2, 2 * part, half), jnp.bfloat16),
            pltpu.VMEM((4, half, part), jnp.bfloat16),
            pltpu.VMEM((2, 2, rows, hidden), jnp.float32),
            pltpu.VMEM((2, rows, hidden), jnp.bfloat16),
            dma((layers, 2)),
            dma((layers, 2)),
            dma((layers, 2)),
            dma((layers, 2)),
            dma((layers, 2)),
            dma((layers, 2)),
            dma((layers,)),
            dma((layers,)),
            dma((layers,)),
            dma((4,)),
            dma((4,)),
            dma((2, 2)),
            dma((2,)),
            dma((2, 4)),
            dma((4,)),
        ],
        compiler_params=pltpu.CompilerParams(vmem_limit_bytes=60 * 1024 * 1024, has_side_effects=True),
        name="stack",
    )(lr, w_up, g_up, w_down, g_down, xt)


def update_kernel(gen_ref, lr_ref, wu, gu, wd, gd, nu, nd):
    is_gen = gen_ref[0] == 1
    lr = lr_ref[0]

    @pl.when(is_gen)
    def _():
        nu[...] = jnp.zeros_like(nu)
        nd[...] = jnp.zeros_like(nd)

    @pl.when(jnp.logical_not(is_gen))
    def _():
        nu[...] = wu[...] - lr * gu[...]
        nd[...] = wd[...] - lr * gd[...]


def update(gen, lr, w_up, g_up, w_down, g_down):
    layers, half, hidden = w_up.shape
    rows = half // 2

    def in_map(l, s, gen_ref, lr_ref):
        live = 1 - gen_ref[0]
        return (l * live, s * live, 0)

    def out_map(l, s, gen_ref, lr_ref):
        return (l, s, 0)

    nbytes = layers * half * hidden * 4 * 6
    return pl.pallas_call(
        update_kernel,
        grid_spec=pltpu.PrefetchScalarGridSpec(
            num_scalar_prefetch=2,
            grid=(layers, 2),
            in_specs=[pl.BlockSpec((1, rows, hidden), in_map)] * 4,
            out_specs=[pl.BlockSpec((1, rows, hidden), out_map)] * 2,
        ),
        out_shape=[jax.ShapeDtypeStruct(w_up.shape, jnp.float32)] * 2,
        cost_estimate=pl.CostEstimate(flops=nbytes * 30, bytes_accessed=nbytes, transcendentals=0),
        name="update",
    )(gen, lr, w_up, g_up, w_down, g_down)


def solution(mesh):
    reps = mesh.shape["rep"]
    axes = ("side", "rep")

    def at(side, rep):
        return side * reps + rep

    pairs = [(t, c) for t in range(2) for c in range(2)]
    up_spec = P("side", None, "rep", None)
    down_spec = P("side", None, None, "rep")
    act_spec = P("side", "rep", None)

    def device_step(w_up, w_down, g_up, g_down, learn_rate, prompts, prompt_lens):
        side = lax.axis_index("side")
        core = lax.axis_index("rep")
        is_gen = side >= 2
        t = lax.rem(side, 2)
        tokens, half = prompts.shape[1], prompts.shape[2]
        part = tokens // 4
        lr = learn_rate.reshape(1)

        w_up, g_up = w_up[0], g_up[0]
        w_down, g_down = jnp.swapaxes(w_down[0], 1, 2), jnp.swapaxes(g_down[0], 1, 2)
        xt = jnp.swapaxes(prompts[0], 0, 1)
        outs = mlp_stack(lr, w_up, g_up, w_down, g_down, xt)[:4]

        back = {}
        for dt in range(2):
            for dc in range(2):
                perm = [(at(a, b), at(2 + (a ^ dt), b ^ dc)) for a, b in pairs]
                back[dt, dc] = lax.ppermute(outs[2 * dt + dc], axes, perm)

        gen = lax.optimization_barrier((is_gen.astype(jnp.int32).reshape(1), outs[0]))[0]
        new_up, new_down = update(gen, lr, w_up, g_up, w_down, g_down)

        by_core = {}
        for dt in range(2):
            lo, hi = back[dt, 0], back[dt, 1]
            by_core[dt] = [jnp.where(core == 0, lo, hi), jnp.where(core == 0, hi, lo)]
        ordered = [jnp.where(t == 0, by_core[0][c], by_core[1][c]) for c in range(2)]
        ordered += [jnp.where(t == 0, by_core[1][c], by_core[0][c]) for c in range(2)]
        y = jnp.concatenate(ordered, axis=1)
        keep = (jnp.arange(tokens)[None, :] < prompt_lens[0]) & is_gen
        y = jnp.swapaxes(jnp.where(keep, y, jnp.zeros_like(y)), 0, 1)
        return new_up[None], jnp.swapaxes(new_down, 1, 2)[None], y[None]

    return jax.shard_map(
        device_step,
        mesh=mesh,
        in_specs=(up_spec, down_spec, up_spec, down_spec, P(), act_spec, P("rep")),
        out_specs=(up_spec, down_spec, act_spec),
        check_vma=False,
    )
```

```python
import jax
import jax.numpy as jnp
from jax import lax
from jax.experimental import pallas as pl
from jax.experimental.pallas import tpu as pltpu
from jax.sharding import PartitionSpec as P


DIRECT = 2
TILE = 512
CHUNK = 1280
UPDATE_SPLIT = 2
LAST = (((1,), (1,)), ((), ()))
GELU_A = 0.7978845608
GELU_B = 0.7978845608 * 0.044715
MESH = pl.DeviceIdType.MESH


def gelu(z):
    t = jnp.tanh(z * (GELU_A + GELU_B * (z * z)))
    h = 0.5 * z
    return h + h * t


def flip(index, by):
    return 1 - index if by else index


def stack_kernel(lr_ref, wu, gu, wd, gd, xt, *refs):
    outs, (own, recv, pown, pfwd), refs = refs[:4], refs[4:8], refs[8:]
    wv, act, xr, fbuf, obuf = refs[:5]
    s_own, r_own, s_main, r_main, s_fwd, r_fwd, s_b, r_b, s_c, s_x, r_x, sem_in, sem_out, sem_ld, sem_y = refs[5:]
    side, core = lax.axis_index("side"), lax.axis_index("rep")
    t = lax.rem(side, 2)
    layers, half, hidden = wu.shape
    rows = half // UPDATE_SPLIT
    part = xt.shape[1] // 4
    spread = part // TILE
    tiles = 2 * spread

    def remote(src, dst, send, recv_sem, to):
        return pltpu.make_async_remote_copy(
            src_ref=src, dst_ref=dst, send_sem=send, recv_sem=recv_sem, device_id=to, device_id_type=MESH
        )

    def x_send(dt, dc, h):
        slot = 2 * dt + dc
        to = (flip(t, dt), flip(core, dc))
        lane = pl.multiple_of((2 * to[0] + to[1]) * part + h * TILE, 128)
        dst = xr.at[slot, :, pl.ds(h * TILE, TILE)]
        return remote(xt.at[:, pl.ds(lane, TILE)], dst, s_x.at[slot, h], r_x.at[slot, h], to)

    def x_recv(dt, tile):
        slot, h = 2 * dt + tile // spread, lax.rem(tile, spread)
        dst = xr.at[slot, :, pl.ds(pl.multiple_of(h * TILE, 128), TILE)]
        return remote(dst, dst, s_x.at[slot, h], r_x.at[slot, h], (t, core))

    def own_copy(l, k):
        return remote(own.at[l, k], pown.at[l, k], s_own.at[l, k], r_own.at[l, k], (t, 1 - core))

    def main_copy(l, k, to_side):
        return remote(own.at[l, k], recv.at[l, k], s_main.at[l, k], r_main.at[l, k], (to_side, core))

    def fwd_copy(l, k):
        return remote(recv.at[l, k], pfwd.at[l, k], s_fwd.at[l, k], r_fwd.at[l, k], (t, 1 - core))

    def b_copy(l):
        return remote(recv.at[l, 1], recv.at[l, 0], s_b.at[l], r_b.at[l], (3 - t, core))

    def c_copy(l):
        return remote(recv.at[l, 0], recv.at[l, 1], s_c.at[l], r_main.at[l, 1], (t, core))

    @pl.when(side >= 2)
    def _():
        for dc in range(2):
            for h in range(spread):
                for dt in range(2):
                    x_send(dt, dc, h).start()

        def hop(l, carry):
            main_copy(l, 1, t).wait_recv()
            b_copy(l).start()

            @pl.when(l > DIRECT)
            def _():
                b_copy(l - 1).wait_recv()
                c_copy(l - 1).start()

            return carry

        lax.fori_loop(DIRECT, layers, hop, 0)
        b_copy(layers - 1).wait_recv()
        c_copy(layers - 1).start()

        def drain(l, carry):
            b_copy(l).wait_send()
            c_copy(l).wait_send()
            return carry

        lax.fori_loop(DIRECT, layers, drain, 0)
        for dc in range(2):
            for h in range(spread):
                for dt in range(2):
                    x_send(dt, dc, h).wait_send()

    @pl.when(side < 2)
    def _():
        lr = lr_ref[0]

        def loads(l, unit):
            k, h = unit // 2, unit % 2
            w, g = ((wu, gu), (wd, gd))[k]
            span = pl.ds(h * rows, rows)
            return (
                pltpu.make_async_copy(w.at[l, span], fbuf.at[h, 0], sem_in.at[h, 0]),
                pltpu.make_async_copy(g.at[l, span], fbuf.at[h, 1], sem_in.at[h, 1]),
            )

        def store(l, unit):
            k, h = unit // 2, unit % 2
            return pltpu.make_async_copy(obuf.at[h], own.at[l, k, pl.ds(h * rows, rows)], sem_out.at[h])

        def send(l, k):
            own_copy(l, k).start()
            if k == 0:
                main_copy(l, 0, 1 - t).start()
                return

            @pl.when(l < DIRECT)
            def _():
                main_copy(l, 1, 1 - t).start()

            @pl.when(l >= DIRECT)
            def _():
                main_copy(l, 1, 2 + t).start()

        for copy in loads(0, 0):
            copy.start()

        def update(l, carry):
            for unit in range(4):
                h = unit % 2
                if unit < 3:
                    for copy in loads(l, unit + 1):
                        copy.start()
                else:

                    @pl.when(l + 1 < layers)
                    def _():
                        for copy in loads(l + 1, 0):
                            copy.start()

                for copy in loads(l, unit):
                    copy.wait()
                if unit >= 2:
                    store(l, unit - 2).wait()
                    if h == 1:
                        send(l, 0)
                else:

                    @pl.when(l > 0)
                    def _():
                        store(l - 1, unit + 2).wait()
                        if h == 1:
                            send(l - 1, 1)

                obuf[h] = (fbuf[h, 0] - lr * fbuf[h, 1]).astype(jnp.bfloat16)
                store(l, unit).start()
            return carry

        lax.fori_loop(0, layers, update, 0)
        store(layers - 1, 2).wait()
        store(layers - 1, 3).wait()
        send(layers - 1, 1)

        twist = lax.rem(core + t, 2)

        def x_in(tile):
            for dt in range(2):
                x_recv(dt, tile).wait_recv()

            def turn(step, carry):
                lane = pl.multiple_of(lax.rem(tile, spread) * TILE + step * 128, 128)
                row = pl.multiple_of(tile * TILE + step * 128, 128)
                for dt in range(2):
                    slot = 2 * dt + tile // spread
                    act[flip(twist, dt), pl.ds(row, 128), :] = jnp.transpose(xr[slot, :, pl.ds(lane, 128)])
                return carry

            lax.fori_loop(0, TILE // 128, turn, 0)

        def fetch(l, k, place):
            src = (own, pown, recv, pfwd)[place]
            slot = lax.rem(l, 2)
            return pltpu.make_async_copy(src.at[l, k], wv.at[slot, k, place], sem_ld.at[k, place])

        def fetch_own(l):
            for k in range(2):
                fetch(l, k, 0).start()
                own_copy(l, k).wait_recv()
                fetch(l, k, 1).start()

        def fetch_recv(l):
            for k in range(2):
                main_copy(l, k, 1 - t).wait_recv()
                fwd_copy(l, k).start()
                fetch(l, k, 2).start()

        def fetch_fwd(l):
            for k in range(2):
                fwd_copy(l, k).wait_recv()
                fetch(l, k, 3).start()

        def fetched(l):
            for k in range(2):
                for place in range(4):
                    fetch(l, k, place).wait()

        fetch_own(0)
        fetch_recv(0)
        fetch_fwd(0)

        def step(index, carry):
            l, tile = index // tiles, index % tiles
            slot = lax.rem(l, 2)

            @pl.when(tile == 0)
            def _():
                @pl.when(l == layers - 1)
                def _():
                    fetch_recv(layers - 1)
                    fetch_fwd(layers - 1)

                fetched(l)

                @pl.when(l + 1 < layers)
                def _():
                    fetch_own(l + 1)

                @pl.when(l + 1 < layers - 1)
                def _():
                    fetch_recv(l + 1)

            @pl.when((tile == tiles // 2) & (l + 1 < layers - 1))
            def _():
                fetch_fwd(l + 1)

            @pl.when(l == 0)
            def _():
                x_in(tile)

            span = pl.ds(pl.multiple_of(tile * TILE, TILE), TILE)
            x0, x1 = act[0, span, :], act[1, span, :]
            acc0 = acc1 = None
            for q in range(2):
                for at in range(0, hidden, CHUNK):
                    cols = pl.ds(at, CHUNK)
                    z = jnp.dot(x0, wv[slot, 0, 2 * q, :, cols], preferred_element_type=jnp.float32)
                    z = z + jnp.dot(x1, wv[slot, 0, 2 * q + 1, :, cols], preferred_element_type=jnp.float32)
                    u = gelu(z).astype(jnp.bfloat16)
                    p0 = lax.dot_general(u, wv[slot, 1, 2 * q, :, cols], LAST, preferred_element_type=jnp.float32)
                    p1 = lax.dot_general(u, wv[slot, 1, 2 * q + 1, :, cols], LAST, preferred_element_type=jnp.float32)
                    acc0 = p0 if acc0 is None else acc0 + p0
                    acc1 = p1 if acc1 is None else acc1 + p1
            act[0, span, :] = (x0.astype(jnp.float32) + acc0).astype(jnp.bfloat16)
            act[1, span, :] = (x1.astype(jnp.float32) + acc1).astype(jnp.bfloat16)
            return carry

        lax.fori_loop(0, layers * tiles, step, 0)

        def x_out(step, carry):
            lane = pl.multiple_of(step * 128, 128)
            for dt in range(2):
                s = flip(twist, dt)
                for dc in range(2):
                    row = pl.multiple_of(dc * part + step * 128, 128)
                    xr[2 * dt + dc, :, pl.ds(lane, 128)] = jnp.transpose(act[s, pl.ds(row, 128), :])
            return carry

        lax.fori_loop(0, part // 128, x_out, 0)
        y_copies = [pltpu.make_async_copy(xr.at[i], outs[i], sem_y.at[i]) for i in range(4)]
        for copy in y_copies:
            copy.start()
        for copy in y_copies:
            copy.wait()

        def drain(l, carry):
            for k in range(2):
                own_copy(l, k).wait_send()
                main_copy(l, k, 1 - t).wait_send()
                fwd_copy(l, k).wait_send()
            return carry

        lax.fori_loop(0, layers, drain, 0)


def mlp_stack(lr, w_up, g_up, w_down, g_down, xt):
    layers, half, hidden = w_up.shape
    part = xt.shape[1] // 4
    rows = half // UPDATE_SPLIT
    dma = pltpu.SemaphoreType.DMA
    any_spec = pl.BlockSpec(memory_space=pl.ANY)
    store = jax.ShapeDtypeStruct((layers, 2, half, hidden), jnp.bfloat16)
    return pl.pallas_call(
        stack_kernel,
        in_specs=[pl.BlockSpec(memory_space=pltpu.SMEM)] + [any_spec] * 5,
        out_specs=[any_spec] * 8,
        out_shape=[jax.ShapeDtypeStruct((half, part), jnp.bfloat16)] * 4 + [store] * 4,
        scratch_shapes=[
            pltpu.VMEM((2, 2, 4, half, hidden), jnp.bfloat16),
            pltpu.VMEM((2, 2 * part, half), jnp.bfloat16),
            pltpu.VMEM((4, half, part), jnp.bfloat16),
            pltpu.VMEM((2, 2, rows, hidden), jnp.float32),
            pltpu.VMEM((2, rows, hidden), jnp.bfloat16),
            dma((layers, 2)),
            dma((layers, 2)),
            dma((layers, 2)),
            dma((layers, 2)),
            dma((layers, 2)),
            dma((layers, 2)),
            dma((layers,)),
            dma((layers,)),
            dma((layers,)),
            dma((4, part // TILE)),
            dma((4, part // TILE)),
            dma((2, 2)),
            dma((2,)),
            dma((2, 4)),
            dma((4,)),
        ],
        compiler_params=pltpu.CompilerParams(vmem_limit_bytes=60 * 1024 * 1024, has_side_effects=True),
        name="stack",
    )(lr, w_up, g_up, w_down, g_down, xt)


def update_kernel(gen_ref, lr_ref, wu, gu, wd, gd, nu, nd):
    is_gen = gen_ref[0] == 1
    lr = lr_ref[0]

    @pl.when(is_gen)
    def _():
        nu[...] = jnp.zeros_like(nu)
        nd[...] = jnp.zeros_like(nd)

    @pl.when(jnp.logical_not(is_gen))
    def _():
        nu[...] = wu[...] - lr * gu[...]
        nd[...] = wd[...] - lr * gd[...]


def update(gen, lr, w_up, g_up, w_down, g_down):
    layers, half, hidden = w_up.shape
    rows = half // 2

    def in_map(l, s, gen_ref, lr_ref):
        live = 1 - gen_ref[0]
        return (l * live, s * live, 0)

    def out_map(l, s, gen_ref, lr_ref):
        return (l, s, 0)

    nbytes = layers * half * hidden * 4 * 6
    return pl.pallas_call(
        update_kernel,
        grid_spec=pltpu.PrefetchScalarGridSpec(
            num_scalar_prefetch=2,
            grid=(layers, 2),
            in_specs=[pl.BlockSpec((1, rows, hidden), in_map)] * 4,
            out_specs=[pl.BlockSpec((1, rows, hidden), out_map)] * 2,
        ),
        out_shape=[jax.ShapeDtypeStruct(w_up.shape, jnp.float32)] * 2,
        cost_estimate=pl.CostEstimate(flops=nbytes * 30, bytes_accessed=nbytes, transcendentals=0),
        name="update",
    )(gen, lr, w_up, g_up, w_down, g_down)


def solution(mesh):
    reps = mesh.shape["rep"]
    axes = ("side", "rep")

    def at(side, rep):
        return side * reps + rep

    pairs = [(t, c) for t in range(2) for c in range(2)]
    up_spec = P("side", None, "rep", None)
    down_spec = P("side", None, None, "rep")
    act_spec = P("side", "rep", None)

    def device_step(w_up, w_down, g_up, g_down, learn_rate, prompts, prompt_lens):
        side = lax.axis_index("side")
        core = lax.axis_index("rep")
        is_gen = side >= 2
        t = lax.rem(side, 2)
        tokens, half = prompts.shape[1], prompts.shape[2]
        part = tokens // 4
        lr = learn_rate.reshape(1)

        w_up, g_up = w_up[0], g_up[0]
        w_down, g_down = jnp.swapaxes(w_down[0], 1, 2), jnp.swapaxes(g_down[0], 1, 2)
        xt = jnp.swapaxes(prompts[0], 0, 1)
        outs = mlp_stack(lr, w_up, g_up, w_down, g_down, xt)[:4]

        back = {}
        for dt in range(2):
            for dc in range(2):
                perm = [(at(a, b), at(2 + (a ^ dt), b ^ dc)) for a, b in pairs]
                back[dt, dc] = lax.ppermute(outs[2 * dt + dc], axes, perm)

        gen = lax.optimization_barrier((is_gen.astype(jnp.int32).reshape(1), outs[0]))[0]
        new_up, new_down = update(gen, lr, w_up, g_up, w_down, g_down)

        by_core = {}
        for dt in range(2):
            lo, hi = back[dt, 0], back[dt, 1]
            by_core[dt] = [jnp.where(core == 0, lo, hi), jnp.where(core == 0, hi, lo)]
        ordered = [jnp.where(t == 0, by_core[0][c], by_core[1][c]) for c in range(2)]
        ordered += [jnp.where(t == 0, by_core[1][c], by_core[0][c]) for c in range(2)]
        y = jnp.concatenate(ordered, axis=1)
        keep = (jnp.arange(tokens)[None, :] < prompt_lens[0]) & is_gen
        y = jnp.swapaxes(jnp.where(keep, y, jnp.zeros_like(y)), 0, 1)
        return new_up[None], jnp.swapaxes(new_down, 1, 2)[None], y[None]

    return jax.shard_map(
        device_step,
        mesh=mesh,
        in_specs=(up_spec, down_spec, up_spec, down_spec, P(), act_spec, P("rep")),
        out_specs=(up_spec, down_spec, act_spec),
        check_vma=False,
    )
```

```python
import jax
import jax.numpy as jnp
from jax import lax
from jax.experimental import pallas as pl
from jax.experimental.pallas import tpu as pltpu
from jax.sharding import PartitionSpec as P


DIRECT = 2
TILE = 512
ARRIVE = 3
UPDATE_SPLIT = 2
LAST = (((1,), (1,)), ((), ()))
GELU_A = 0.7978845608
GELU_B = 0.7978845608 * 0.044715
MESH = pl.DeviceIdType.MESH


def gelu(z):
    t = jnp.tanh(z * (GELU_A + GELU_B * (z * z)))
    h = 0.5 * z
    return h + h * t


def flip(index, by):
    return 1 - index if by else index


def stack_kernel(lr_ref, wu, gu, wd, gd, xt, *refs):
    outs, (own, recv, pown, pfwd), refs = refs[:4], refs[4:8], refs[8:]
    wv, act, xr, psum, fbuf, obuf = refs[:6]
    s_own, r_own, s_main, r_main, s_fwd, r_fwd, s_b, r_b, s_c, s_x, r_x, sem_in, sem_out, sem_ld, sem_y = refs[6:]
    side, core = lax.axis_index("side"), lax.axis_index("rep")
    t = lax.rem(side, 2)
    layers, half, hidden = wu.shape
    rows = half // UPDATE_SPLIT
    part = xt.shape[1] // 4
    spread = part // TILE
    tiles = 2 * spread

    def remote(src, dst, send, recv_sem, to):
        return pltpu.make_async_remote_copy(
            src_ref=src, dst_ref=dst, send_sem=send, recv_sem=recv_sem, device_id=to, device_id_type=MESH
        )

    def x_send(dt, dc, h):
        slot = 2 * dt + dc
        to = (flip(t, dt), flip(core, dc))
        lane = pl.multiple_of((2 * to[0] + to[1]) * part + h * TILE, 128)
        dst = xr.at[slot, :, pl.ds(h * TILE, TILE)]
        return remote(xt.at[:, pl.ds(lane, TILE)], dst, s_x.at[slot, h], r_x.at[slot, h], to)

    def x_recv(dt, tile):
        slot, h = 2 * dt + tile // spread, lax.rem(tile, spread)
        dst = xr.at[slot, :, pl.ds(pl.multiple_of(h * TILE, 128), TILE)]
        return remote(dst, dst, s_x.at[slot, h], r_x.at[slot, h], (t, core))

    def own_copy(l, k):
        return remote(own.at[l, k], pown.at[l, k], s_own.at[l, k], r_own.at[l, k], (t, 1 - core))

    def main_copy(l, k, to_side):
        return remote(own.at[l, k], recv.at[l, k], s_main.at[l, k], r_main.at[l, k], (to_side, core))

    def fwd_copy(l, k):
        return remote(recv.at[l, k], pfwd.at[l, k], s_fwd.at[l, k], r_fwd.at[l, k], (t, 1 - core))

    def b_copy(l):
        return remote(recv.at[l, 1], recv.at[l, 0], s_b.at[l], r_b.at[l], (3 - t, core))

    def c_copy(l):
        return remote(recv.at[l, 0], recv.at[l, 1], s_c.at[l], r_main.at[l, 1], (t, core))

    @pl.when(side >= 2)
    def _():
        for dc in range(2):
            for h in range(spread):
                for dt in range(2):
                    x_send(dt, dc, h).start()

        def hop(l, carry):
            main_copy(l, 1, t).wait_recv()
            b_copy(l).start()

            @pl.when(l > DIRECT)
            def _():
                b_copy(l - 1).wait_recv()
                c_copy(l - 1).start()

            return carry

        lax.fori_loop(DIRECT, layers, hop, 0)
        b_copy(layers - 1).wait_recv()
        c_copy(layers - 1).start()

        def drain(l, carry):
            b_copy(l).wait_send()
            c_copy(l).wait_send()
            return carry

        lax.fori_loop(DIRECT, layers, drain, 0)
        for dc in range(2):
            for h in range(spread):
                for dt in range(2):
                    x_send(dt, dc, h).wait_send()

    @pl.when(side < 2)
    def _():
        lr = lr_ref[0]

        def loads(l, unit):
            k, h = unit // 2, unit % 2
            w, g = ((wu, gu), (wd, gd))[k]
            span = pl.ds(h * rows, rows)
            return (
                pltpu.make_async_copy(w.at[l, span], fbuf.at[h, 0], sem_in.at[h, 0]),
                pltpu.make_async_copy(g.at[l, span], fbuf.at[h, 1], sem_in.at[h, 1]),
            )

        def store(l, unit):
            k, h = unit // 2, unit % 2
            return pltpu.make_async_copy(obuf.at[h], own.at[l, k, pl.ds(h * rows, rows)], sem_out.at[h])

        def send(l, k):
            own_copy(l, k).start()
            if k == 0:
                main_copy(l, 0, 1 - t).start()
                return

            @pl.when(l < DIRECT)
            def _():
                main_copy(l, 1, 1 - t).start()

            @pl.when(l >= DIRECT)
            def _():
                main_copy(l, 1, 2 + t).start()

        for copy in loads(0, 0):
            copy.start()

        def update(l, carry):
            for unit in range(4):
                h = unit % 2
                if unit < 3:
                    for copy in loads(l, unit + 1):
                        copy.start()
                else:

                    @pl.when(l + 1 < layers)
                    def _():
                        for copy in loads(l + 1, 0):
                            copy.start()

                for copy in loads(l, unit):
                    copy.wait()
                if unit >= 2:
                    store(l, unit - 2).wait()
                    if h == 1:
                        send(l, 0)
                else:

                    @pl.when(l > 0)
                    def _():
                        store(l - 1, unit + 2).wait()
                        if h == 1:
                            send(l - 1, 1)

                obuf[h] = (fbuf[h, 0] - lr * fbuf[h, 1]).astype(jnp.bfloat16)
                store(l, unit).start()
            return carry

        lax.fori_loop(0, layers, update, 0)
        store(layers - 1, 2).wait()
        store(layers - 1, 3).wait()
        send(layers - 1, 1)

        twist = lax.rem(core + t, 2)

        def x_in(tile):
            for dt in range(2):
                x_recv(dt, tile).wait_recv()

            def turn(step, carry):
                lane = pl.multiple_of(lax.rem(tile, spread) * TILE + step * 128, 128)
                row = pl.multiple_of(tile * TILE + step * 128, 128)
                for dt in range(2):
                    slot = 2 * dt + tile // spread
                    act[flip(twist, dt), pl.ds(row, 128), :] = jnp.transpose(xr[slot, :, pl.ds(lane, 128)])
                return carry

            lax.fori_loop(0, TILE // 128, turn, 0)

        def fetch(l, k, place):
            src = (own, pown, recv, pfwd)[place]
            slot = lax.rem(l, 2)
            return pltpu.make_async_copy(src.at[l, k], wv.at[slot, k, place], sem_ld.at[k, place])

        def fetch_own(l):
            for k in range(2):
                fetch(l, k, 0).start()
                own_copy(l, k).wait_recv()
                fetch(l, k, 1).start()

        def fetch_recv(l):
            for k in range(2):
                main_copy(l, k, 1 - t).wait_recv()
                fwd_copy(l, k).start()
                fetch(l, k, 2).start()

        def fetch_fwd(l):
            for k in range(2):
                fwd_copy(l, k).wait_recv()
                fetch(l, k, 3).start()

        def fetched(l, q):
            for k in range(2):
                for place in (2 * q, 2 * q + 1):
                    fetch(l, k, place).wait()

        def half_tile(l, q, tile):
            slot = lax.rem(l, 2)
            span = pl.ds(pl.multiple_of(tile * TILE, TILE), TILE)
            x0, x1 = act[0, span, :], act[1, span, :]
            z = jnp.dot(x0, wv[slot, 0, 2 * q], preferred_element_type=jnp.float32)
            z = z + jnp.dot(x1, wv[slot, 0, 2 * q + 1], preferred_element_type=jnp.float32)
            u = gelu(z).astype(jnp.bfloat16)
            p0 = lax.dot_general(u, wv[slot, 1, 2 * q], LAST, preferred_element_type=jnp.float32)
            p1 = lax.dot_general(u, wv[slot, 1, 2 * q + 1], LAST, preferred_element_type=jnp.float32)
            return span, (x0, x1), (p0, p1)

        def x_out(tile):
            def turn(step, carry):
                lane = pl.multiple_of(lax.rem(tile, spread) * TILE + step * 128, 128)
                row = pl.multiple_of(tile * TILE + step * 128, 128)
                for dt in range(2):
                    slot = 2 * dt + tile // spread
                    xr[slot, :, pl.ds(lane, 128)] = jnp.transpose(act[flip(twist, dt), pl.ds(row, 128), :])
                return carry

            lax.fori_loop(0, TILE // 128, turn, 0)

        fetch_own(0)

        def layer(l, carry):
            fetched(l, 0)

            @pl.when(l + 1 < layers)
            def _():
                fetch_own(l + 1)

            def first(tile, carry):
                @pl.when(l == 0)
                def _():
                    x_in(tile)

                @pl.when(tile == ARRIVE)
                def _():
                    fetch_recv(l)

                span, _, sums = half_tile(l, 0, tile)
                for s in range(2):
                    psum[s, span, :] = sums[s]
                return carry

            lax.fori_loop(0, tiles, first, 0)
            fetch_fwd(l)
            fetched(l, 1)

            def second(tile, carry):
                span, xs, sums = half_tile(l, 1, tile)
                for s in range(2):
                    total = psum[s, span, :] + sums[s]
                    act[s, span, :] = (xs[s].astype(jnp.float32) + total).astype(jnp.bfloat16)

                @pl.when(l == layers - 1)
                def _():
                    x_out(tile)

                return carry

            lax.fori_loop(0, tiles, second, 0)
            return carry

        lax.fori_loop(0, layers, layer, 0)

        y_copies = [pltpu.make_async_copy(xr.at[i], outs[i], sem_y.at[i]) for i in range(4)]
        for copy in y_copies:
            copy.start()
        for copy in y_copies:
            copy.wait()

        def drain(l, carry):
            for k in range(2):
                own_copy(l, k).wait_send()
                main_copy(l, k, 1 - t).wait_send()
                fwd_copy(l, k).wait_send()
            return carry

        lax.fori_loop(0, layers, drain, 0)


def mlp_stack(lr, w_up, g_up, w_down, g_down, xt):
    layers, half, hidden = w_up.shape
    part = xt.shape[1] // 4
    rows = half // UPDATE_SPLIT
    dma = pltpu.SemaphoreType.DMA
    any_spec = pl.BlockSpec(memory_space=pl.ANY)
    store = jax.ShapeDtypeStruct((layers, 2, half, hidden), jnp.bfloat16)
    return pl.pallas_call(
        stack_kernel,
        in_specs=[pl.BlockSpec(memory_space=pltpu.SMEM)] + [any_spec] * 5,
        out_specs=[any_spec] * 8,
        out_shape=[jax.ShapeDtypeStruct((half, part), jnp.bfloat16)] * 4 + [store] * 4,
        scratch_shapes=[
            pltpu.VMEM((2, 2, 4, half, hidden), jnp.bfloat16),
            pltpu.VMEM((2, 2 * part, half), jnp.bfloat16),
            pltpu.VMEM((4, half, part), jnp.bfloat16),
            pltpu.VMEM((2, 2 * part, half), jnp.float32),
            pltpu.VMEM((2, 2, rows, hidden), jnp.float32),
            pltpu.VMEM((2, rows, hidden), jnp.bfloat16),
            dma((layers, 2)),
            dma((layers, 2)),
            dma((layers, 2)),
            dma((layers, 2)),
            dma((layers, 2)),
            dma((layers, 2)),
            dma((layers,)),
            dma((layers,)),
            dma((layers,)),
            dma((4, part // TILE)),
            dma((4, part // TILE)),
            dma((2, 2)),
            dma((2,)),
            dma((2, 4)),
            dma((4,)),
        ],
        compiler_params=pltpu.CompilerParams(vmem_limit_bytes=60 * 1024 * 1024, has_side_effects=True),
        name="stack",
    )(lr, w_up, g_up, w_down, g_down, xt)


def update_kernel(gen_ref, lr_ref, wu, gu, wd, gd, nu, nd):
    is_gen = gen_ref[0] == 1
    lr = lr_ref[0]

    @pl.when(is_gen)
    def _():
        nu[...] = jnp.zeros_like(nu)
        nd[...] = jnp.zeros_like(nd)

    @pl.when(jnp.logical_not(is_gen))
    def _():
        nu[...] = wu[...] - lr * gu[...]
        nd[...] = wd[...] - lr * gd[...]


def update(gen, lr, w_up, g_up, w_down, g_down):
    layers, half, hidden = w_up.shape
    rows = half // 2

    def in_map(l, s, gen_ref, lr_ref):
        live = 1 - gen_ref[0]
        return (l * live, s * live, 0)

    def out_map(l, s, gen_ref, lr_ref):
        return (l, s, 0)

    nbytes = layers * half * hidden * 4 * 6
    return pl.pallas_call(
        update_kernel,
        grid_spec=pltpu.PrefetchScalarGridSpec(
            num_scalar_prefetch=2,
            grid=(layers, 2),
            in_specs=[pl.BlockSpec((1, rows, hidden), in_map)] * 4,
            out_specs=[pl.BlockSpec((1, rows, hidden), out_map)] * 2,
        ),
        out_shape=[jax.ShapeDtypeStruct(w_up.shape, jnp.float32)] * 2,
        cost_estimate=pl.CostEstimate(flops=nbytes * 30, bytes_accessed=nbytes, transcendentals=0),
        name="update",
    )(gen, lr, w_up, g_up, w_down, g_down)


def solution(mesh):
    reps = mesh.shape["rep"]
    axes = ("side", "rep")

    def at(side, rep):
        return side * reps + rep

    pairs = [(t, c) for t in range(2) for c in range(2)]
    up_spec = P("side", None, "rep", None)
    down_spec = P("side", None, None, "rep")
    act_spec = P("side", "rep", None)

    def device_step(w_up, w_down, g_up, g_down, learn_rate, prompts, prompt_lens):
        side = lax.axis_index("side")
        core = lax.axis_index("rep")
        is_gen = side >= 2
        t = lax.rem(side, 2)
        tokens, half = prompts.shape[1], prompts.shape[2]
        part = tokens // 4
        lr = learn_rate.reshape(1)

        w_up, g_up = w_up[0], g_up[0]
        w_down, g_down = jnp.swapaxes(w_down[0], 1, 2), jnp.swapaxes(g_down[0], 1, 2)
        xt = jnp.swapaxes(prompts[0], 0, 1)
        outs = mlp_stack(lr, w_up, g_up, w_down, g_down, xt)[:4]

        back = {}
        for dt in range(2):
            for dc in range(2):
                perm = [(at(a, b), at(2 + (a ^ dt), b ^ dc)) for a, b in pairs]
                back[dt, dc] = lax.ppermute(outs[2 * dt + dc], axes, perm)

        gen = lax.optimization_barrier((is_gen.astype(jnp.int32).reshape(1), outs[0]))[0]
        new_up, new_down = update(gen, lr, w_up, g_up, w_down, g_down)

        by_core = {}
        for dt in range(2):
            lo, hi = back[dt, 0], back[dt, 1]
            by_core[dt] = [jnp.where(core == 0, lo, hi), jnp.where(core == 0, hi, lo)]
        ordered = [jnp.where(t == 0, by_core[0][c], by_core[1][c]) for c in range(2)]
        ordered += [jnp.where(t == 0, by_core[1][c], by_core[0][c]) for c in range(2)]
        y = jnp.concatenate(ordered, axis=1)
        keep = (jnp.arange(tokens)[None, :] < prompt_lens[0]) & is_gen
        y = jnp.swapaxes(jnp.where(keep, y, jnp.zeros_like(y)), 0, 1)
        return new_up[None], jnp.swapaxes(new_down, 1, 2)[None], y[None]

    return jax.shard_map(
        device_step,
        mesh=mesh,
        in_specs=(up_spec, down_spec, up_spec, down_spec, P(), act_spec, P("rep")),
        out_specs=(up_spec, down_spec, act_spec),
        check_vma=False,
    )
```

```python
import jax
import jax.numpy as jnp
from jax import lax
from jax.experimental import pallas as pl
from jax.experimental.pallas import tpu as pltpu
from jax.sharding import PartitionSpec as P


HAND = 10
DIRECT = 2
TILE = 512
ARRIVE = 3
UPDATE_SPLIT = 2
LAST = (((1,), (1,)), ((), ()))
GELU_A = 0.7978845608
GELU_B = 0.7978845608 * 0.044715
MESH = pl.DeviceIdType.MESH


def gelu(z):
    t = jnp.tanh(z * (GELU_A + GELU_B * (z * z)))
    h = 0.5 * z
    return h + h * t


def flip(index, by):
    return 1 - index if by else index


def stack_kernel(lr_ref, wu, gu, wd, gd, xt, *refs):
    outs, yin, (own, recv, pown, pfwd), refs = refs[:2], refs[2], refs[3:7], refs[7:]
    wv, act, xr, psum, fbuf, obuf = refs[:6]
    s_own, r_own, s_main, r_main, s_fwd, r_fwd, s_a, s_b, r_b, s_c, s_x, r_x, s_h, r_h, s_y, r_y = refs[6:22]
    sem_in, sem_out, sem_ld, sem_y = refs[22:]
    side, core = lax.axis_index("side"), lax.axis_index("rep")
    t = lax.rem(side, 2)
    layers, half, hidden = wu.shape
    rows = half // UPDATE_SPLIT
    part = xt.shape[1] // 4
    spread = part // TILE
    tiles = 2 * spread

    def remote(src, dst, send, recv_sem, to):
        return pltpu.make_async_remote_copy(
            src_ref=src, dst_ref=dst, send_sem=send, recv_sem=recv_sem, device_id=to, device_id_type=MESH
        )

    def x_send(dt, dc, h):
        slot = 2 * dt + dc
        to = (flip(t, dt), flip(core, dc))
        lane = pl.multiple_of((2 * to[0] + to[1]) * part + h * TILE, 128)
        dst = xr.at[slot, :, pl.ds(h * TILE, TILE)]
        return remote(xt.at[:, pl.ds(lane, TILE)], dst, s_x.at[slot, h], r_x.at[slot, h], to)

    def x_recv(dt, tile):
        slot, h = 2 * dt + tile // spread, lax.rem(tile, spread)
        dst = xr.at[slot, :, pl.ds(pl.multiple_of(h * TILE, 128), TILE)]
        return remote(dst, dst, s_x.at[slot, h], r_x.at[slot, h], (t, core))

    def own_copy(l, k):
        return remote(own.at[l, k], pown.at[l, k], s_own.at[l, k], r_own.at[l, k], (side, 1 - core))

    def fwd_copy(l, k):
        return remote(recv.at[l, k], pfwd.at[l, k], s_fwd.at[l, k], r_fwd.at[l, k], (side, 1 - core))

    def main_copy(l, k):
        return remote(own.at[l, k], recv.at[l, k], s_main.at[l, k], r_main.at[l, k], (1 - t, core))

    def a_copy(l, k):
        sent = s_main.at[l, 1] if k else s_a.at[l]
        return remote(own.at[l, k], own.at[l, k], sent, r_main.at[l, k], (2 + t, core))

    def b_copy(l, k):
        return remote(own.at[l, k], recv.at[l, k], s_b.at[l, k], r_b.at[l, k], (3 - t, core))

    def c_copy(l):
        return remote(recv.at[l, 1], recv.at[l, 1], s_c.at[l], r_main.at[l, 1], (t, core))

    def h_copy(tile, s):
        rows_of = act.at[s, pl.ds(pl.multiple_of(tile * TILE, TILE), TILE)]
        return remote(rows_of, rows_of, s_h.at[tile, s], r_h.at[tile, s], (2 + t, core))

    def y_copy(tile):
        lanes = pl.ds(pl.multiple_of(tile * TILE, TILE), TILE)
        return remote(xr.at[2, :, lanes], yin.at[t, :, lanes], s_y.at[tile], r_y.at[tile], (3 - t, core))

    def y_arrival(tile):
        lanes = pl.ds(pl.multiple_of(tile * TILE, TILE), TILE)
        dst = yin.at[1 - t, :, lanes]
        return remote(dst, dst, s_y.at[tile], r_y.at[tile], (3 - t, core))

    def y_keep(tile):
        lanes = pl.ds(pl.multiple_of(tile * TILE, TILE), TILE)
        return pltpu.make_async_copy(xr.at[0, :, lanes], yin.at[t, :, lanes], sem_y.at[tile])

    twist = lax.rem(core + t, 2)

    def fetch(l, k, place):
        src = (own, pown, recv, pfwd)[place]
        slot = lax.rem(l, 2)
        return pltpu.make_async_copy(src.at[l, k], wv.at[slot, k, place], sem_ld.at[k, place])

    def fetched(l, q):
        for k in range(2):
            for place in (2 * q, 2 * q + 1):
                fetch(l, k, place).wait()

    def half_tile(l, q, tile):
        slot = lax.rem(l, 2)
        span = pl.ds(pl.multiple_of(tile * TILE, TILE), TILE)
        x0, x1 = act[0, span, :], act[1, span, :]
        z = jnp.dot(x0, wv[slot, 0, 2 * q], preferred_element_type=jnp.float32)
        z = z + jnp.dot(x1, wv[slot, 0, 2 * q + 1], preferred_element_type=jnp.float32)
        u = gelu(z).astype(jnp.bfloat16)
        p0 = lax.dot_general(u, wv[slot, 1, 2 * q], LAST, preferred_element_type=jnp.float32)
        p1 = lax.dot_general(u, wv[slot, 1, 2 * q + 1], LAST, preferred_element_type=jnp.float32)
        return span, (x0, x1), (p0, p1)

    def x_out(tile):
        def turn(step, carry):
            lane = pl.multiple_of(lax.rem(tile, spread) * TILE + step * 128, 128)
            row = pl.multiple_of(tile * TILE + step * 128, 128)
            for dt in range(2):
                slot = 2 * dt + tile // spread
                xr[slot, :, pl.ds(lane, 128)] = jnp.transpose(act[flip(twist, dt), pl.ds(row, 128), :])
            return carry

        lax.fori_loop(0, TILE // 128, turn, 0)

    def first_half(l, tile):
        span, _, sums = half_tile(l, 0, tile)
        for s in range(2):
            psum[s, span, :] = sums[s]

    def second_half(l, tile):
        span, xs, sums = half_tile(l, 1, tile)
        for s in range(2):
            total = psum[s, span, :] + sums[s]
            act[s, span, :] = (xs[s].astype(jnp.float32) + total).astype(jnp.bfloat16)

    @pl.when(side >= 2)
    def _():
        for dc in range(2):
            for h in range(spread):
                for dt in range(2):
                    x_send(dt, dc, h).start()

        def relay(l):
            b_copy(l, 1).wait_recv()
            c_copy(l).start()

            @pl.when(l >= HAND)
            def _():
                fwd_copy(l, 1).start()

        def hop(l, carry):
            a_copy(l, 1).wait_recv()
            b_copy(l, 1).start()

            @pl.when(l >= HAND)
            def _():
                own_copy(l, 1).start()

            @pl.when(l > DIRECT)
            def _():
                relay(l - 1)

            return carry

        lax.fori_loop(DIRECT, layers, hop, 0)
        relay(layers - 1)
        for l in range(HAND, layers):
            a_copy(l, 0).wait_recv()
            b_copy(l, 0).start()
            own_copy(l, 0).start()
        for l in range(HAND, layers):
            b_copy(l, 0).wait_recv()
            fwd_copy(l, 0).start()
        for l in range(HAND, layers):
            for k in range(2):
                own_copy(l, k).wait_recv()
                fwd_copy(l, k).wait_recv()
                for place in range(4):
                    fetch(l, k, place).start()
            fetched(l, 0)
            fetched(l, 1)

        def finish(tile, carry):
            for s in range(2):
                h_copy(tile, s).wait_recv()

            def layer(l, carry):
                first_half(l, tile)
                second_half(l, tile)
                return carry

            lax.fori_loop(HAND, layers, layer, 0)
            x_out(tile)
            y_copy(tile).start()
            y_keep(tile).start()
            return carry

        lax.fori_loop(0, spread, finish, 0)

        def drain(l, carry):
            b_copy(l, 1).wait_send()
            c_copy(l).wait_send()
            return carry

        lax.fori_loop(DIRECT, layers, drain, 0)
        for l in range(HAND, layers):
            b_copy(l, 0).wait_send()
            for k in range(2):
                own_copy(l, k).wait_send()
                fwd_copy(l, k).wait_send()
        for tile in range(spread):
            y_keep(tile).wait()
            y_copy(tile).wait_send()
            y_arrival(tile).wait_recv()
        for dc in range(2):
            for h in range(spread):
                for dt in range(2):
                    x_send(dt, dc, h).wait_send()

    @pl.when(side < 2)
    def _():
        lr = lr_ref[0]

        def loads(l, unit):
            k, h = unit // 2, unit % 2
            w, g = ((wu, gu), (wd, gd))[k]
            span = pl.ds(h * rows, rows)
            return (
                pltpu.make_async_copy(w.at[l, span], fbuf.at[h, 0], sem_in.at[h, 0]),
                pltpu.make_async_copy(g.at[l, span], fbuf.at[h, 1], sem_in.at[h, 1]),
            )

        def store(l, unit):
            k, h = unit // 2, unit % 2
            return pltpu.make_async_copy(obuf.at[h], own.at[l, k, pl.ds(h * rows, rows)], sem_out.at[h])

        def send(l, k):
            own_copy(l, k).start()
            if k == 0:
                main_copy(l, 0).start()
                return

            @pl.when(l < DIRECT)
            def _():
                main_copy(l, 1).start()

            @pl.when(l >= DIRECT)
            def _():
                a_copy(l, 1).start()

        for copy in loads(0, 0):
            copy.start()

        def update(l, carry):
            for unit in range(4):
                h = unit % 2
                if unit < 3:
                    for copy in loads(l, unit + 1):
                        copy.start()
                else:

                    @pl.when(l + 1 < layers)
                    def _():
                        for copy in loads(l + 1, 0):
                            copy.start()

                for copy in loads(l, unit):
                    copy.wait()
                if unit >= 2:
                    store(l, unit - 2).wait()
                    if h == 1:
                        send(l, 0)
                else:

                    @pl.when(l > 0)
                    def _():
                        store(l - 1, unit + 2).wait()
                        if h == 1:
                            send(l - 1, 1)

                obuf[h] = (fbuf[h, 0] - lr * fbuf[h, 1]).astype(jnp.bfloat16)
                store(l, unit).start()
            return carry

        lax.fori_loop(0, layers, update, 0)
        store(layers - 1, 2).wait()
        store(layers - 1, 3).wait()
        send(layers - 1, 1)
        for l in range(HAND, layers):
            a_copy(l, 0).start()

        def x_in(tile):
            for dt in range(2):
                x_recv(dt, tile).wait_recv()

            def turn(step, carry):
                lane = pl.multiple_of(lax.rem(tile, spread) * TILE + step * 128, 128)
                row = pl.multiple_of(tile * TILE + step * 128, 128)
                for dt in range(2):
                    slot = 2 * dt + tile // spread
                    act[flip(twist, dt), pl.ds(row, 128), :] = jnp.transpose(xr[slot, :, pl.ds(lane, 128)])
                return carry

            lax.fori_loop(0, TILE // 128, turn, 0)

        def fetch_own(l):
            for k in range(2):
                fetch(l, k, 0).start()
                own_copy(l, k).wait_recv()
                fetch(l, k, 1).start()

        def fetch_recv(l):
            for k in range(2):
                main_copy(l, k).wait_recv()
                fwd_copy(l, k).start()
                fetch(l, k, 2).start()

        def fetch_fwd(l):
            for k in range(2):
                fwd_copy(l, k).wait_recv()
                fetch(l, k, 3).start()

        fetch_own(0)

        def layer(l, carry):
            fetched(l, 0)

            @pl.when(l + 1 < layers)
            def _():
                fetch_own(l + 1)

            def first(tile, carry):
                @pl.when(l == 0)
                def _():
                    x_in(tile)

                @pl.when(tile == ARRIVE)
                def _():
                    fetch_recv(l)

                first_half(l, tile)
                return carry

            start = spread * (l // HAND)
            lax.fori_loop(start, tiles, first, 0)
            fetch_fwd(l)
            fetched(l, 1)

            def second(tile, carry):
                @pl.when((l == HAND - 1) & (tile >= 1) & (tile <= spread))
                def _():
                    for s in range(2):
                        h_copy(tile - 1, s).start()

                second_half(l, tile)

                @pl.when(l == layers - 1)
                def _():
                    x_out(tile)

                return carry

            lax.fori_loop(start, tiles, second, 0)
            return carry

        lax.fori_loop(0, layers, layer, 0)

        y_copies = [pltpu.make_async_copy(xr.at[2 * dt + 1], outs[dt], sem_y.at[dt]) for dt in range(2)]
        for copy in y_copies:
            copy.start()
        for copy in y_copies:
            copy.wait()

        def drain(l, carry):
            for k in range(2):
                own_copy(l, k).wait_send()
                main_copy(l, k).wait_send()
                fwd_copy(l, k).wait_send()
            return carry

        lax.fori_loop(0, layers, drain, 0)
        for l in range(HAND, layers):
            a_copy(l, 0).wait_send()
        for tile in range(spread):
            for s in range(2):
                h_copy(tile, s).wait_send()


def mlp_stack(lr, w_up, g_up, w_down, g_down, xt):
    layers, half, hidden = w_up.shape
    part = xt.shape[1] // 4
    rows = half // UPDATE_SPLIT
    dma = pltpu.SemaphoreType.DMA
    any_spec = pl.BlockSpec(memory_space=pl.ANY)
    store = jax.ShapeDtypeStruct((layers, 2, half, hidden), jnp.bfloat16)
    return pl.pallas_call(
        stack_kernel,
        in_specs=[pl.BlockSpec(memory_space=pltpu.SMEM)] + [any_spec] * 5,
        out_specs=[any_spec] * 7,
        out_shape=[jax.ShapeDtypeStruct((half, part), jnp.bfloat16)] * 2
        + [jax.ShapeDtypeStruct((2, half, part), jnp.bfloat16)]
        + [store] * 4,
        scratch_shapes=[
            pltpu.VMEM((2, 2, 4, half, hidden), jnp.bfloat16),
            pltpu.VMEM((2, 2 * part, half), jnp.bfloat16),
            pltpu.VMEM((4, half, part), jnp.bfloat16),
            pltpu.VMEM((2, 2 * part, half), jnp.float32),
            pltpu.VMEM((2, 2, rows, hidden), jnp.float32),
            pltpu.VMEM((2, rows, hidden), jnp.bfloat16),
            dma((layers, 2)),
            dma((layers, 2)),
            dma((layers, 2)),
            dma((layers, 2)),
            dma((layers, 2)),
            dma((layers, 2)),
            dma((layers,)),
            dma((layers, 2)),
            dma((layers, 2)),
            dma((layers,)),
            dma((4, part // TILE)),
            dma((4, part // TILE)),
            dma((part // TILE, 2)),
            dma((part // TILE, 2)),
            dma((part // TILE,)),
            dma((part // TILE,)),
            dma((2, 2)),
            dma((2,)),
            dma((2, 4)),
            dma((part // TILE,)),
        ],
        compiler_params=pltpu.CompilerParams(vmem_limit_bytes=60 * 1024 * 1024, has_side_effects=True),
        name="stack",
    )(lr, w_up, g_up, w_down, g_down, xt)


def update_kernel(gen_ref, lr_ref, wu, gu, wd, gd, nu, nd):
    is_gen = gen_ref[0] == 1
    lr = lr_ref[0]

    @pl.when(is_gen)
    def _():
        nu[...] = jnp.zeros_like(nu)
        nd[...] = jnp.zeros_like(nd)

    @pl.when(jnp.logical_not(is_gen))
    def _():
        nu[...] = wu[...] - lr * gu[...]
        nd[...] = wd[...] - lr * gd[...]


def update(gen, lr, w_up, g_up, w_down, g_down):
    layers, half, hidden = w_up.shape
    rows = half // 2

    def in_map(l, s, gen_ref, lr_ref):
        live = 1 - gen_ref[0]
        return (l * live, s * live, 0)

    def out_map(l, s, gen_ref, lr_ref):
        return (l, s, 0)

    nbytes = layers * half * hidden * 4 * 6
    return pl.pallas_call(
        update_kernel,
        grid_spec=pltpu.PrefetchScalarGridSpec(
            num_scalar_prefetch=2,
            grid=(layers, 2),
            in_specs=[pl.BlockSpec((1, rows, hidden), in_map)] * 4,
            out_specs=[pl.BlockSpec((1, rows, hidden), out_map)] * 2,
        ),
        out_shape=[jax.ShapeDtypeStruct(w_up.shape, jnp.float32)] * 2,
        cost_estimate=pl.CostEstimate(flops=nbytes * 30, bytes_accessed=nbytes, transcendentals=0),
        name="update",
    )(gen, lr, w_up, g_up, w_down, g_down)


def solution(mesh):
    reps = mesh.shape["rep"]
    axes = ("side", "rep")

    def at(side, rep):
        return side * reps + rep

    pairs = [(t, c) for t in range(2) for c in range(2)]
    up_spec = P("side", None, "rep", None)
    down_spec = P("side", None, None, "rep")
    act_spec = P("side", "rep", None)

    def device_step(w_up, w_down, g_up, g_down, learn_rate, prompts, prompt_lens):
        side = lax.axis_index("side")
        core = lax.axis_index("rep")
        is_gen = side >= 2
        t = lax.rem(side, 2)
        tokens, half = prompts.shape[1], prompts.shape[2]
        part = tokens // 4
        lr = learn_rate.reshape(1)

        w_up, g_up = w_up[0], g_up[0]
        w_down, g_down = jnp.swapaxes(w_down[0], 1, 2), jnp.swapaxes(g_down[0], 1, 2)
        xt = jnp.swapaxes(prompts[0], 0, 1)
        *outs, mine = mlp_stack(lr, w_up, g_up, w_down, g_down, xt)[:3]

        back = []
        for dt in range(2):
            perm = [(at(a, b), at(2 + (a ^ dt), 1 - b)) for a, b in pairs]
            back.append(lax.ppermute(outs[dt], axes, perm))

        gen = lax.optimization_barrier((is_gen.astype(jnp.int32).reshape(1), outs[0]))[0]
        new_up, new_down = update(gen, lr, w_up, g_up, w_down, g_down)

        pieces = []
        for tj in range(2):
            theirs = jnp.where(t == tj, back[0], back[1])
            pieces += [jnp.where(core == cj, mine[tj], theirs) for cj in range(2)]
        y = jnp.concatenate(pieces, axis=1)
        keep = (jnp.arange(tokens)[None, :] < prompt_lens[0]) & is_gen
        y = jnp.swapaxes(jnp.where(keep, y, jnp.zeros_like(y)), 0, 1)
        return new_up[None], jnp.swapaxes(new_down, 1, 2)[None], y[None]

    return jax.shard_map(
        device_step,
        mesh=mesh,
        in_specs=(up_spec, down_spec, up_spec, down_spec, P(), act_spec, P("rep")),
        out_specs=(up_spec, down_spec, act_spec),
        check_vma=False,
    )
```

```python
import functools

import jax
import jax.numpy as jnp
from jax import lax
from jax.experimental import pallas as pl
from jax.experimental.pallas import tpu as pltpu
from jax.sharding import PartitionSpec as P


HAND = 10
DIRECT = 2
TILE = 512
ARRIVE = 3
UPDATE_SPLIT = 2
EARLY = 2
LAST = (((1,), (1,)), ((), ()))
GELU_A = 0.7978845608
GELU_B = 0.7978845608 * 0.044715
MESH = pl.DeviceIdType.MESH


def gelu(z):
    t = jnp.tanh(z * (GELU_A + GELU_B * (z * z)))
    h = 0.5 * z
    return h + h * t


def flip(index, by):
    return 1 - index if by else index


def stack_kernel(lr_ref, wu, gu, wd, gd, xt, *refs):
    outs, (yin, zin, raw), (own, recv, pown, pfwd), refs = refs[:2], refs[2:5], refs[5:9], refs[9:]
    wv, act, xr, psum, fbuf, obuf = refs[:6]
    s_own, r_own, s_main, r_main, s_fwd, r_fwd, s_a, s_b, r_b, s_c, s_x, r_x, s_h, r_h, s_y, r_y, s_z, r_z = refs[6:24]
    sem_in, sem_out, sem_raw, sem_ld, sem_y = refs[24:]
    side, core = lax.axis_index("side"), lax.axis_index("rep")
    t = lax.rem(side, 2)
    layers, half, hidden = wu.shape
    rows = half // UPDATE_SPLIT
    part = xt.shape[1] // 4
    spread = part // TILE
    tiles = 2 * spread

    def remote(src, dst, send, recv_sem, to):
        return pltpu.make_async_remote_copy(
            src_ref=src, dst_ref=dst, send_sem=send, recv_sem=recv_sem, device_id=to, device_id_type=MESH
        )

    def x_send(dt, dc, h):
        slot = 2 * dt + dc
        to = (flip(t, dt), flip(core, dc))
        lane = pl.multiple_of((2 * to[0] + to[1]) * part + h * TILE, 128)
        dst = xr.at[slot, :, pl.ds(h * TILE, TILE)]
        return remote(xt.at[:, pl.ds(lane, TILE)], dst, s_x.at[slot, h], r_x.at[slot, h], to)

    def x_recv(dt, tile):
        slot, h = 2 * dt + tile // spread, lax.rem(tile, spread)
        dst = xr.at[slot, :, pl.ds(pl.multiple_of(h * TILE, 128), TILE)]
        return remote(dst, dst, s_x.at[slot, h], r_x.at[slot, h], (t, core))

    def own_copy(l, k):
        return remote(own.at[l, k], pown.at[l, k], s_own.at[l, k], r_own.at[l, k], (side, 1 - core))

    def fwd_copy(l, k):
        return remote(recv.at[l, k], pfwd.at[l, k], s_fwd.at[l, k], r_fwd.at[l, k], (side, 1 - core))

    def main_copy(l, k):
        return remote(own.at[l, k], recv.at[l, k], s_main.at[l, k], r_main.at[l, k], (1 - t, core))

    def a_copy(l, k):
        sent = s_main.at[l, 1] if k else s_a.at[l]
        return remote(own.at[l, k], own.at[l, k], sent, r_main.at[l, k], (2 + t, core))

    def b_copy(l, k):
        return remote(own.at[l, k], recv.at[l, k], s_b.at[l, k], r_b.at[l, k], (3 - t, core))

    def c_copy(l):
        return remote(recv.at[l, 1], recv.at[l, 1], s_c.at[l], r_main.at[l, 1], (t, core))

    def h_copy(tile, s):
        rows_of = act.at[s, pl.ds(pl.multiple_of(tile * TILE, TILE), TILE)]
        return remote(rows_of, rows_of, s_h.at[tile, s], r_h.at[tile, s], (2 + t, core))

    def y_copy(tile):
        lanes = pl.ds(pl.multiple_of(tile * TILE, TILE), TILE)
        return remote(xr.at[2, :, lanes], yin.at[t, :, lanes], s_y.at[tile], r_y.at[tile], (3 - t, core))

    def y_arrival(tile):
        lanes = pl.ds(pl.multiple_of(tile * TILE, TILE), TILE)
        dst = yin.at[1 - t, :, lanes]
        return remote(dst, dst, s_y.at[tile], r_y.at[tile], (3 - t, core))

    def y_keep(tile):
        lanes = pl.ds(pl.multiple_of(tile * TILE, TILE), TILE)
        return pltpu.make_async_copy(xr.at[0, :, lanes], yin.at[t, :, lanes], sem_y.at[tile])

    def z_copy(dt):
        lanes = pl.ds(0, part - TILE)
        src, dst = xr.at[2 * dt + 1, :, lanes], zin.at[t]
        return remote(src, dst, s_z.at[dt], r_z.at[t], (2 + flip(t, dt), 1 - core))

    def z_arrival(tj):
        return remote(zin.at[tj], zin.at[tj], s_z.at[0], r_z.at[tj], (tj, 1 - core))

    twist = lax.rem(core + t, 2)

    def fetch(l, k, place):
        src = (own, pown, recv, pfwd)[place]
        slot = lax.rem(l, 2)
        return pltpu.make_async_copy(src.at[l, k], wv.at[slot, k, place], sem_ld.at[k, place])

    def fetched(l, q):
        for k in range(2):
            for place in (2 * q, 2 * q + 1):
                fetch(l, k, place).wait()

    def half_tile(l, q, tile):
        slot = lax.rem(l, 2)
        span = pl.ds(pl.multiple_of(tile * TILE, TILE), TILE)
        x0, x1 = act[0, span, :], act[1, span, :]
        z = jnp.dot(x0, wv[slot, 0, 2 * q], preferred_element_type=jnp.float32)
        z = z + jnp.dot(x1, wv[slot, 0, 2 * q + 1], preferred_element_type=jnp.float32)
        u = gelu(z).astype(jnp.bfloat16)
        p0 = lax.dot_general(u, wv[slot, 1, 2 * q], LAST, preferred_element_type=jnp.float32)
        p1 = lax.dot_general(u, wv[slot, 1, 2 * q + 1], LAST, preferred_element_type=jnp.float32)
        return span, (x0, x1), (p0, p1)

    def x_out(tile):
        def turn(step, carry):
            lane = pl.multiple_of(lax.rem(tile, spread) * TILE + step * 128, 128)
            row = pl.multiple_of(tile * TILE + step * 128, 128)
            for dt in range(2):
                slot = 2 * dt + tile // spread
                xr[slot, :, pl.ds(lane, 128)] = jnp.transpose(act[flip(twist, dt), pl.ds(row, 128), :])
            return carry

        lax.fori_loop(0, TILE // 128, turn, 0)

    def first_half(l, tile):
        span, _, sums = half_tile(l, 0, tile)
        for s in range(2):
            psum[s, span, :] = sums[s]

    def second_half(l, tile):
        span, xs, sums = half_tile(l, 1, tile)
        for s in range(2):
            total = psum[s, span, :] + sums[s]
            act[s, span, :] = (xs[s].astype(jnp.float32) + total).astype(jnp.bfloat16)

    @pl.when(side >= 2)
    def _():
        for dc in range(2):
            for h in range(spread):
                for dt in range(2):
                    x_send(dt, dc, h).start()

        def relay(l):
            b_copy(l, 1).wait_recv()
            c_copy(l).start()

            @pl.when(l >= HAND)
            def _():
                fwd_copy(l, 1).start()

        def hop(l, carry):
            a_copy(l, 1).wait_recv()
            b_copy(l, 1).start()

            @pl.when(l >= HAND)
            def _():
                own_copy(l, 1).start()

            @pl.when(l > DIRECT)
            def _():
                relay(l - 1)

            return carry

        lax.fori_loop(DIRECT, layers, hop, 0)
        relay(layers - 1)
        for l in range(HAND, layers):
            a_copy(l, 0).wait_recv()
            b_copy(l, 0).start()
            own_copy(l, 0).start()
        for l in range(HAND, layers):
            b_copy(l, 0).wait_recv()
            fwd_copy(l, 0).start()
        for l in range(HAND, layers):
            for k in range(2):
                own_copy(l, k).wait_recv()
                fwd_copy(l, k).wait_recv()
                for place in range(4):
                    fetch(l, k, place).start()
            fetched(l, 0)
            fetched(l, 1)

        def finish(tile, carry):
            for s in range(2):
                h_copy(tile, s).wait_recv()

            def layer(l, carry):
                first_half(l, tile)
                second_half(l, tile)
                return carry

            lax.fori_loop(HAND, layers, layer, 0)
            x_out(tile)
            y_copy(tile).start()
            y_keep(tile).start()
            return carry

        lax.fori_loop(0, spread, finish, 0)

        def drain(l, carry):
            b_copy(l, 1).wait_send()
            c_copy(l).wait_send()
            return carry

        lax.fori_loop(DIRECT, layers, drain, 0)
        for l in range(HAND, layers):
            b_copy(l, 0).wait_send()
            for k in range(2):
                own_copy(l, k).wait_send()
                fwd_copy(l, k).wait_send()
        for tile in range(spread):
            y_keep(tile).wait()
            y_copy(tile).wait_send()
            y_arrival(tile).wait_recv()
        for tj in range(2):
            z_arrival(tj).wait_recv()
        for dc in range(2):
            for h in range(spread):
                for dt in range(2):
                    x_send(dt, dc, h).wait_send()

    @pl.when(side < 2)
    def _():
        lr = lr_ref[0]

        def loads(l, unit):
            k, h = unit // 2, unit % 2
            w, g = ((wu, gu), (wd, gd))[k]
            span = pl.ds(h * rows, rows)
            return (
                pltpu.make_async_copy(w.at[l, span], fbuf.at[unit, 0], sem_in.at[unit, 0]),
                pltpu.make_async_copy(g.at[l, span], fbuf.at[unit, 1], sem_in.at[unit, 1]),
            )

        def raw_store(l, unit):
            k, h = unit // 2, unit % 2
            return pltpu.make_async_copy(fbuf.at[unit, 0], raw.at[l, k, pl.ds(h * rows, rows)], sem_raw.at[unit])

        def store(l, unit):
            k, h = unit // 2, unit % 2
            return pltpu.make_async_copy(obuf.at[h], own.at[l, k, pl.ds(h * rows, rows)], sem_out.at[h])

        def send(l, k):
            own_copy(l, k).start()
            if k == 0:
                main_copy(l, 0).start()
                return

            @pl.when(l < DIRECT)
            def _():
                main_copy(l, 1).start()

            @pl.when(l >= DIRECT)
            def _():
                a_copy(l, 1).start()

        for unit in range(2):
            for copy in loads(0, unit):
                copy.start()

        def update(l, carry):
            for unit in range(4):
                h = unit % 2
                ahead = (unit + 2) % 4
                if unit < 2:

                    @pl.when(l > 0)
                    def _():
                        raw_store(l - 1, ahead).wait()

                    for copy in loads(l, ahead):
                        copy.start()
                else:

                    @pl.when(l + 1 < layers)
                    def _():
                        raw_store(l, ahead).wait()
                        for copy in loads(l + 1, ahead):
                            copy.start()

                for copy in loads(l, unit):
                    copy.wait()
                if unit >= 2:
                    store(l, unit - 2).wait()
                    if h == 1:
                        send(l, 0)
                else:

                    @pl.when(l > 0)
                    def _():
                        store(l - 1, unit + 2).wait()
                        if h == 1:
                            send(l - 1, 1)

                new = fbuf[unit, 0] - lr * fbuf[unit, 1]
                fbuf[unit, 0] = new
                obuf[h] = new.astype(jnp.bfloat16)
                raw_store(l, unit).start()
                store(l, unit).start()
            return carry

        lax.fori_loop(0, layers, update, 0)
        store(layers - 1, 2).wait()
        store(layers - 1, 3).wait()
        for unit in range(4):
            raw_store(layers - 1, unit).wait()
        send(layers - 1, 1)
        for l in range(HAND, layers):
            a_copy(l, 0).start()

        def x_in(tile):
            for dt in range(2):
                x_recv(dt, tile).wait_recv()

            def turn(step, carry):
                lane = pl.multiple_of(lax.rem(tile, spread) * TILE + step * 128, 128)
                row = pl.multiple_of(tile * TILE + step * 128, 128)
                for dt in range(2):
                    slot = 2 * dt + tile // spread
                    act[flip(twist, dt), pl.ds(row, 128), :] = jnp.transpose(xr[slot, :, pl.ds(lane, 128)])
                return carry

            lax.fori_loop(0, TILE // 128, turn, 0)

        def fetch_own(l):
            for k in range(2):
                fetch(l, k, 0).start()
                own_copy(l, k).wait_recv()
                fetch(l, k, 1).start()

        def fetch_recv(l):
            for k in range(2):
                main_copy(l, k).wait_recv()
                fwd_copy(l, k).start()
                fetch(l, k, 2).start()

        def fetch_fwd(l):
            for k in range(2):
                fwd_copy(l, k).wait_recv()
                fetch(l, k, 3).start()

        fetch_own(0)

        def layer(l, carry):
            fetched(l, 0)

            @pl.when(l + 1 < layers)
            def _():
                fetch_own(l + 1)

            def first(tile, carry):
                @pl.when(l == 0)
                def _():
                    x_in(tile)

                @pl.when(tile == ARRIVE)
                def _():
                    fetch_recv(l)

                first_half(l, tile)
                return carry

            start = spread * (l // HAND)
            lax.fori_loop(start, tiles, first, 0)
            fetch_fwd(l)
            fetched(l, 1)

            def second(tile, carry):
                @pl.when((l == HAND - 1) & (tile >= 1) & (tile <= spread))
                def _():
                    for s in range(2):
                        h_copy(tile - 1, s).start()

                second_half(l, tile)

                @pl.when(l == layers - 1)
                def _():
                    x_out(tile)

                @pl.when((l == layers - 1) & (tile == tiles - 2))
                def _():
                    for dt in range(2):
                        z_copy(dt).start()

                return carry

            lax.fori_loop(start, tiles, second, 0)
            return carry

        lax.fori_loop(0, layers, layer, 0)

        lanes = pl.ds(part - TILE, TILE)
        y_copies = [pltpu.make_async_copy(xr.at[2 * dt + 1, :, lanes], outs[dt], sem_y.at[dt]) for dt in range(2)]
        for copy in y_copies:
            copy.start()
        for copy in y_copies:
            copy.wait()

        def drain(l, carry):
            for k in range(2):
                own_copy(l, k).wait_send()
                main_copy(l, k).wait_send()
                fwd_copy(l, k).wait_send()
            return carry

        lax.fori_loop(0, layers, drain, 0)
        for l in range(HAND, layers):
            a_copy(l, 0).wait_send()
        for tile in range(spread):
            for s in range(2):
                h_copy(tile, s).wait_send()
        for dt in range(2):
            z_copy(dt).wait_send()


def mlp_stack(lr, w_up, g_up, w_down, g_down, xt):
    layers, half, hidden = w_up.shape
    part = xt.shape[1] // 4
    rows = half // UPDATE_SPLIT
    dma = pltpu.SemaphoreType.DMA
    any_spec = pl.BlockSpec(memory_space=pl.ANY)
    store = jax.ShapeDtypeStruct((layers, 2, half, hidden), jnp.bfloat16)
    return pl.pallas_call(
        stack_kernel,
        in_specs=[pl.BlockSpec(memory_space=pltpu.SMEM)] + [any_spec] * 5,
        out_specs=[any_spec] * 9,
        out_shape=[jax.ShapeDtypeStruct((half, TILE), jnp.bfloat16)] * 2
        + [jax.ShapeDtypeStruct((2, half, lanes), jnp.bfloat16) for lanes in (part, part - TILE)]
        + [jax.ShapeDtypeStruct((layers, 2, half, hidden), jnp.float32)]
        + [store] * 4,
        scratch_shapes=[
            pltpu.VMEM((2, 2, 4, half, hidden), jnp.bfloat16),
            pltpu.VMEM((2, 2 * part, half), jnp.bfloat16),
            pltpu.VMEM((4, half, part), jnp.bfloat16),
            pltpu.VMEM((2, 2 * part, half), jnp.float32),
            pltpu.VMEM((4, 2, rows, hidden), jnp.float32),
            pltpu.VMEM((2, rows, hidden), jnp.bfloat16),
            dma((layers, 2)),
            dma((layers, 2)),
            dma((layers, 2)),
            dma((layers, 2)),
            dma((layers, 2)),
            dma((layers, 2)),
            dma((layers,)),
            dma((layers, 2)),
            dma((layers, 2)),
            dma((layers,)),
            dma((4, part // TILE)),
            dma((4, part // TILE)),
            dma((part // TILE, 2)),
            dma((part // TILE, 2)),
            dma((part // TILE,)),
            dma((part // TILE,)),
            dma((2,)),
            dma((2,)),
            dma((4, 2)),
            dma((2,)),
            dma((4,)),
            dma((2, 4)),
            dma((part // TILE,)),
        ],
        compiler_params=pltpu.CompilerParams(vmem_limit_bytes=60 * 1024 * 1024, has_side_effects=True),
        name="stack",
    )(lr, w_up, g_up, w_down, g_down, xt)


def place_kernel(gen_ref, raw, *refs, first):
    nu, nd = refs[-2:]
    is_gen = gen_ref[0] == 1

    @pl.when(is_gen)
    def _():
        nu[...] = jnp.zeros_like(nu)
        nd[...] = jnp.zeros_like(nd)

    @pl.when(jnp.logical_not(is_gen) & (pl.program_id(0) >= first))
    def _():
        nu[...] = raw[:, 0]
        nd[...] = raw[:, 1]


def place_update(gen, raw, prev, first, last):
    layers, _, half, hidden = raw.shape
    rows = half // 2
    final = last == layers

    def trainer_at(l, s):
        live = l >= first
        return jnp.where(live, l, first), jnp.where(live, s, 0)

    def in_map(l, s, gen_ref):
        l, s = trainer_at(l, s)
        live = 1 - gen_ref[0]
        return (l * live, 0, s * live, 0)

    def out_map(l, s, gen_ref):
        own_l, own_s = trainer_at(l, s)
        is_gen = gen_ref[0] == 1
        gen_l, gen_s = (l, s) if final else (0, 0)
        return (jnp.where(is_gen, gen_l, own_l), jnp.where(is_gen, gen_s, own_s), 0)

    shape = jax.ShapeDtypeStruct((layers, half, hidden), jnp.float32)
    prev = list(prev or ())
    nbytes = (last - first) * half * hidden * 4 * 4
    return pl.pallas_call(
        functools.partial(place_kernel, first=first),
        grid_spec=pltpu.PrefetchScalarGridSpec(
            num_scalar_prefetch=1,
            grid=(last, 2),
            in_specs=[pl.BlockSpec((1, 2, rows, hidden), in_map)] + [pl.BlockSpec(memory_space=pl.ANY)] * len(prev),
            out_specs=[pl.BlockSpec((1, rows, hidden), out_map)] * 2,
        ),
        out_shape=[shape] * 2,
        input_output_aliases={2: 0, 3: 1} if prev else {},
        cost_estimate=pl.CostEstimate(flops=nbytes * 30, bytes_accessed=nbytes, transcendentals=0),
        name="place",
    )(gen, raw, *prev)


def solution(mesh):
    reps = mesh.shape["rep"]
    axes = ("side", "rep")

    def at(side, rep):
        return side * reps + rep

    pairs = [(t, c) for t in range(2) for c in range(2)]
    up_spec = P("side", None, "rep", None)
    down_spec = P("side", None, None, "rep")
    act_spec = P("side", "rep", None)

    def device_step(w_up, w_down, g_up, g_down, learn_rate, prompts, prompt_lens):
        side = lax.axis_index("side")
        core = lax.axis_index("rep")
        is_gen = side >= 2
        t = lax.rem(side, 2)
        tokens, half = prompts.shape[1], prompts.shape[2]
        part = tokens // 4
        lr = learn_rate.reshape(1)

        w_up, g_up = w_up[0], g_up[0]
        w_down, g_down = jnp.swapaxes(w_down[0], 1, 2), jnp.swapaxes(g_down[0], 1, 2)
        xt = jnp.swapaxes(prompts[0], 0, 1)
        *outs, mine, theirs, raw = mlp_stack(lr, w_up, g_up, w_down, g_down, xt)[:5]
        gen = is_gen.astype(jnp.int32).reshape(1)
        layers = raw.shape[0]
        placed = place_update(gen, raw, None, 0, EARLY)
        outs = lax.optimization_barrier((*outs, *placed))[:2]

        back = []
        for dt in range(2):
            perm = [(at(a, b), at(2 + (a ^ dt), 1 - b)) for a, b in pairs]
            back.append(lax.ppermute(outs[dt], axes, perm))

        new_up, new_down = place_update(gen, raw, placed, EARLY, layers)

        pieces = []
        for tj in range(2):
            handed = jnp.concatenate([theirs[tj], jnp.where(t == tj, back[0], back[1])], axis=1)
            pieces += [jnp.where(core == cj, mine[tj], handed) for cj in range(2)]
        y = jnp.concatenate(pieces, axis=1)
        keep = (jnp.arange(tokens)[None, :] < prompt_lens[0]) & is_gen
        y = jnp.swapaxes(jnp.where(keep, y, jnp.zeros_like(y)), 0, 1)
        return new_up[None], jnp.swapaxes(new_down, 1, 2)[None], y[None]

    return jax.shard_map(
        device_step,
        mesh=mesh,
        in_specs=(up_spec, down_spec, up_spec, down_spec, P(), act_spec, P("rep")),
        out_specs=(up_spec, down_spec, act_spec),
        check_vma=False,
    )
```

```python
import functools

import jax
import jax.numpy as jnp
from jax import lax
from jax.experimental import pallas as pl
from jax.experimental.pallas import tpu as pltpu
from jax.sharding import PartitionSpec as P


HAND = 10
DIRECT = 2
TILE = 512
ARRIVE = 3
UPDATE_SPLIT = 2
PLACE_SLOTS = 8
EARLY = 2
LAST = (((1,), (1,)), ((), ()))
GELU_A = 0.7978845608
GELU_B = 0.7978845608 * 0.044715
MESH = pl.DeviceIdType.MESH


def gelu(z):
    t = jnp.tanh(z * (GELU_A + GELU_B * (z * z)))
    h = 0.5 * z
    return h + h * t


def flip(index, by):
    return 1 - index if by else index


def stack_kernel(lr_ref, wu, gu, wd, gd, xt, *refs):
    outs, (yin, zin, raw), (own, recv, pown, pfwd), refs = refs[:2], refs[2:5], refs[5:9], refs[9:]
    wv, act, xr, psum, fbuf, obuf = refs[:6]
    s_own, r_own, s_main, r_main, s_fwd, r_fwd, s_a, s_b, r_b, s_c, s_x, r_x, s_h, r_h, s_y, r_y, s_z, r_z = refs[6:24]
    sem_in, sem_out, sem_raw, sem_ld, sem_y = refs[24:]
    side, core = lax.axis_index("side"), lax.axis_index("rep")
    t = lax.rem(side, 2)
    layers, half, hidden = wu.shape
    rows = half // UPDATE_SPLIT
    part = xt.shape[1] // 4
    spread = part // TILE
    tiles = 2 * spread

    def remote(src, dst, send, recv_sem, to):
        return pltpu.make_async_remote_copy(
            src_ref=src, dst_ref=dst, send_sem=send, recv_sem=recv_sem, device_id=to, device_id_type=MESH
        )

    def x_send(dt, dc, h):
        slot = 2 * dt + dc
        to = (flip(t, dt), flip(core, dc))
        lane = pl.multiple_of((2 * to[0] + to[1]) * part + h * TILE, 128)
        dst = xr.at[slot, :, pl.ds(h * TILE, TILE)]
        return remote(xt.at[:, pl.ds(lane, TILE)], dst, s_x.at[slot, h], r_x.at[slot, h], to)

    def x_recv(dt, tile):
        slot, h = 2 * dt + tile // spread, lax.rem(tile, spread)
        dst = xr.at[slot, :, pl.ds(pl.multiple_of(h * TILE, 128), TILE)]
        return remote(dst, dst, s_x.at[slot, h], r_x.at[slot, h], (t, core))

    def own_copy(l, k):
        return remote(own.at[l, k], pown.at[l, k], s_own.at[l, k], r_own.at[l, k], (side, 1 - core))

    def fwd_copy(l, k):
        return remote(recv.at[l, k], pfwd.at[l, k], s_fwd.at[l, k], r_fwd.at[l, k], (side, 1 - core))

    def main_copy(l, k):
        return remote(own.at[l, k], recv.at[l, k], s_main.at[l, k], r_main.at[l, k], (1 - t, core))

    def a_copy(l, k):
        sent = s_main.at[l, 1] if k else s_a.at[l]
        return remote(own.at[l, k], own.at[l, k], sent, r_main.at[l, k], (2 + t, core))

    def b_copy(l, k):
        return remote(own.at[l, k], recv.at[l, k], s_b.at[l, k], r_b.at[l, k], (3 - t, core))

    def c_copy(l):
        return remote(recv.at[l, 1], recv.at[l, 1], s_c.at[l], r_main.at[l, 1], (t, core))

    def h_copy(tile, s):
        rows_of = act.at[s, pl.ds(pl.multiple_of(tile * TILE, TILE), TILE)]
        return remote(rows_of, rows_of, s_h.at[tile, s], r_h.at[tile, s], (2 + t, core))

    def y_copy(tile):
        lanes = pl.ds(pl.multiple_of(tile * TILE, TILE), TILE)
        return remote(xr.at[2, :, lanes], yin.at[t, :, lanes], s_y.at[tile], r_y.at[tile], (3 - t, core))

    def y_arrival(tile):
        lanes = pl.ds(pl.multiple_of(tile * TILE, TILE), TILE)
        dst = yin.at[1 - t, :, lanes]
        return remote(dst, dst, s_y.at[tile], r_y.at[tile], (3 - t, core))

    def y_keep(tile):
        lanes = pl.ds(pl.multiple_of(tile * TILE, TILE), TILE)
        return pltpu.make_async_copy(xr.at[0, :, lanes], yin.at[t, :, lanes], sem_y.at[tile])

    def z_copy(dt):
        lanes = pl.ds(0, part - TILE)
        src, dst = xr.at[2 * dt + 1, :, lanes], zin.at[t]
        return remote(src, dst, s_z.at[dt], r_z.at[t], (2 + flip(t, dt), 1 - core))

    def z_arrival(tj):
        return remote(zin.at[tj], zin.at[tj], s_z.at[0], r_z.at[tj], (tj, 1 - core))

    twist = lax.rem(core + t, 2)

    def fetch(l, k, place):
        src = (own, pown, recv, pfwd)[place]
        slot = lax.rem(l, 2)
        return pltpu.make_async_copy(src.at[l, k], wv.at[slot, k, place], sem_ld.at[k, place])

    def fetched(l, q):
        for k in range(2):
            for place in (2 * q, 2 * q + 1):
                fetch(l, k, place).wait()

    def half_tile(l, q, tile):
        slot = lax.rem(l, 2)
        span = pl.ds(pl.multiple_of(tile * TILE, TILE), TILE)
        x0, x1 = act[0, span, :], act[1, span, :]
        z = jnp.dot(x0, wv[slot, 0, 2 * q], preferred_element_type=jnp.float32)
        z = z + jnp.dot(x1, wv[slot, 0, 2 * q + 1], preferred_element_type=jnp.float32)
        u = gelu(z).astype(jnp.bfloat16)
        p0 = lax.dot_general(u, wv[slot, 1, 2 * q], LAST, preferred_element_type=jnp.float32)
        p1 = lax.dot_general(u, wv[slot, 1, 2 * q + 1], LAST, preferred_element_type=jnp.float32)
        return span, (x0, x1), (p0, p1)

    def x_out(tile):
        def turn(step, carry):
            lane = pl.multiple_of(lax.rem(tile, spread) * TILE + step * 128, 128)
            row = pl.multiple_of(tile * TILE + step * 128, 128)
            for dt in range(2):
                slot = 2 * dt + tile // spread
                xr[slot, :, pl.ds(lane, 128)] = jnp.transpose(act[flip(twist, dt), pl.ds(row, 128), :])
            return carry

        lax.fori_loop(0, TILE // 128, turn, 0)

    def first_half(l, tile):
        span, _, sums = half_tile(l, 0, tile)
        for s in range(2):
            psum[s, span, :] = sums[s]

    def second_half(l, tile):
        span, xs, sums = half_tile(l, 1, tile)
        for s in range(2):
            total = psum[s, span, :] + sums[s]
            act[s, span, :] = (xs[s].astype(jnp.float32) + total).astype(jnp.bfloat16)

    @pl.when(side >= 2)
    def _():
        for dc in range(2):
            for h in range(spread):
                for dt in range(2):
                    x_send(dt, dc, h).start()

        def relay(l):
            b_copy(l, 1).wait_recv()
            c_copy(l).start()

            @pl.when(l >= HAND)
            def _():
                fwd_copy(l, 1).start()

        def hop(l, carry):
            a_copy(l, 1).wait_recv()
            b_copy(l, 1).start()

            @pl.when(l >= HAND)
            def _():
                own_copy(l, 1).start()

            @pl.when(l > DIRECT)
            def _():
                relay(l - 1)

            return carry

        lax.fori_loop(DIRECT, layers, hop, 0)
        relay(layers - 1)
        for l in range(HAND, layers):
            a_copy(l, 0).wait_recv()
            b_copy(l, 0).start()
            own_copy(l, 0).start()
        for l in range(HAND, layers):
            b_copy(l, 0).wait_recv()
            fwd_copy(l, 0).start()
        for l in range(HAND, layers):
            for k in range(2):
                own_copy(l, k).wait_recv()
                fwd_copy(l, k).wait_recv()
                for place in range(4):
                    fetch(l, k, place).start()
            fetched(l, 0)
            fetched(l, 1)

        def finish(tile, carry):
            for s in range(2):
                h_copy(tile, s).wait_recv()

            def layer(l, carry):
                first_half(l, tile)
                second_half(l, tile)
                return carry

            lax.fori_loop(HAND, layers, layer, 0)
            x_out(tile)
            y_copy(tile).start()
            y_keep(tile).start()
            return carry

        lax.fori_loop(0, spread, finish, 0)

        def drain(l, carry):
            b_copy(l, 1).wait_send()
            c_copy(l).wait_send()
            return carry

        lax.fori_loop(DIRECT, layers, drain, 0)
        for l in range(HAND, layers):
            b_copy(l, 0).wait_send()
            for k in range(2):
                own_copy(l, k).wait_send()
                fwd_copy(l, k).wait_send()
        for tile in range(spread):
            y_keep(tile).wait()
            y_copy(tile).wait_send()
            y_arrival(tile).wait_recv()
        for tj in range(2):
            z_arrival(tj).wait_recv()
        for dc in range(2):
            for h in range(spread):
                for dt in range(2):
                    x_send(dt, dc, h).wait_send()

    @pl.when(side < 2)
    def _():
        lr = lr_ref[0]

        def loads(l, unit):
            k, h = unit // 2, unit % 2
            w, g = ((wu, gu), (wd, gd))[k]
            span = pl.ds(h * rows, rows)
            return (
                pltpu.make_async_copy(w.at[l, span], fbuf.at[unit, 0], sem_in.at[unit, 0]),
                pltpu.make_async_copy(g.at[l, span], fbuf.at[unit, 1], sem_in.at[unit, 1]),
            )

        def raw_store(l, unit):
            k, h = unit // 2, unit % 2
            return pltpu.make_async_copy(fbuf.at[unit, 0], raw.at[l, k, pl.ds(h * rows, rows)], sem_raw.at[unit])

        def store(l, unit):
            k, h = unit // 2, unit % 2
            return pltpu.make_async_copy(obuf.at[h], own.at[l, k, pl.ds(h * rows, rows)], sem_out.at[h])

        def send(l, k):
            own_copy(l, k).start()
            if k == 0:
                main_copy(l, 0).start()
                return

            @pl.when(l < DIRECT)
            def _():
                main_copy(l, 1).start()

            @pl.when(l >= DIRECT)
            def _():
                a_copy(l, 1).start()

        for unit in range(2):
            for copy in loads(0, unit):
                copy.start()

        def update(l, carry):
            for unit in range(4):
                h = unit % 2
                ahead = (unit + 2) % 4
                if unit < 2:

                    @pl.when(l > 0)
                    def _():
                        raw_store(l - 1, ahead).wait()

                    for copy in loads(l, ahead):
                        copy.start()
                else:

                    @pl.when(l + 1 < layers)
                    def _():
                        raw_store(l, ahead).wait()
                        for copy in loads(l + 1, ahead):
                            copy.start()

                for copy in loads(l, unit):
                    copy.wait()
                if unit >= 2:
                    store(l, unit - 2).wait()
                    if h == 1:
                        send(l, 0)
                else:

                    @pl.when(l > 0)
                    def _():
                        store(l - 1, unit + 2).wait()
                        if h == 1:
                            send(l - 1, 1)

                new = fbuf[unit, 0] - lr * fbuf[unit, 1]
                fbuf[unit, 0] = new
                obuf[h] = new.astype(jnp.bfloat16)
                raw_store(l, unit).start()
                store(l, unit).start()
            return carry

        lax.fori_loop(0, layers, update, 0)
        store(layers - 1, 2).wait()
        store(layers - 1, 3).wait()
        for unit in range(4):
            raw_store(layers - 1, unit).wait()
        send(layers - 1, 1)
        for l in range(HAND, layers):
            a_copy(l, 0).start()

        def x_in(tile):
            for dt in range(2):
                x_recv(dt, tile).wait_recv()

            def turn(step, carry):
                lane = pl.multiple_of(lax.rem(tile, spread) * TILE + step * 128, 128)
                row = pl.multiple_of(tile * TILE + step * 128, 128)
                for dt in range(2):
                    slot = 2 * dt + tile // spread
                    act[flip(twist, dt), pl.ds(row, 128), :] = jnp.transpose(xr[slot, :, pl.ds(lane, 128)])
                return carry

            lax.fori_loop(0, TILE // 128, turn, 0)

        def fetch_own(l):
            for k in range(2):
                fetch(l, k, 0).start()
                own_copy(l, k).wait_recv()
                fetch(l, k, 1).start()

        def fetch_recv(l):
            for k in (1, 0):
                main_copy(l, k).wait_recv()
                fwd_copy(l, k).start()
                fetch(l, k, 2).start()

        def fetch_fwd(l):
            for k in (1, 0):
                fwd_copy(l, k).wait_recv()
                fetch(l, k, 3).start()

        fetch_own(0)

        def layer(l, carry):
            fetched(l, 0)

            @pl.when(l + 1 < layers)
            def _():
                fetch_own(l + 1)

            def first(tile, carry):
                @pl.when(l == 0)
                def _():
                    x_in(tile)

                @pl.when(tile == ARRIVE)
                def _():
                    fetch_recv(l)

                first_half(l, tile)
                return carry

            start = spread * (l // HAND)
            lax.fori_loop(start, tiles, first, 0)
            fetch_fwd(l)
            fetched(l, 1)

            def second(tile, carry):
                @pl.when((l == HAND - 1) & (tile >= 1) & (tile <= spread))
                def _():
                    for s in range(2):
                        h_copy(tile - 1, s).start()

                second_half(l, tile)

                @pl.when(l == layers - 1)
                def _():
                    x_out(tile)

                @pl.when((l == layers - 1) & (tile == tiles - 2))
                def _():
                    for dt in range(2):
                        z_copy(dt).start()

                return carry

            lax.fori_loop(start, tiles, second, 0)
            return carry

        lax.fori_loop(0, layers, layer, 0)

        lanes = pl.ds(part - TILE, TILE)
        y_copies = [pltpu.make_async_copy(xr.at[2 * dt + 1, :, lanes], outs[dt], sem_y.at[dt]) for dt in range(2)]
        for copy in y_copies:
            copy.start()
        for copy in y_copies:
            copy.wait()

        def drain(l, carry):
            for k in range(2):
                own_copy(l, k).wait_send()
                main_copy(l, k).wait_send()
                fwd_copy(l, k).wait_send()
            return carry

        lax.fori_loop(0, layers, drain, 0)
        for l in range(HAND, layers):
            a_copy(l, 0).wait_send()
        for tile in range(spread):
            for s in range(2):
                h_copy(tile, s).wait_send()
        for dt in range(2):
            z_copy(dt).wait_send()


def mlp_stack(lr, w_up, g_up, w_down, g_down, xt):
    layers, half, hidden = w_up.shape
    part = xt.shape[1] // 4
    rows = half // UPDATE_SPLIT
    dma = pltpu.SemaphoreType.DMA
    any_spec = pl.BlockSpec(memory_space=pl.ANY)
    store = jax.ShapeDtypeStruct((layers, 2, half, hidden), jnp.bfloat16)
    return pl.pallas_call(
        stack_kernel,
        in_specs=[pl.BlockSpec(memory_space=pltpu.SMEM)] + [any_spec] * 5,
        out_specs=[any_spec] * 9,
        out_shape=[jax.ShapeDtypeStruct((half, TILE), jnp.bfloat16)] * 2
        + [jax.ShapeDtypeStruct((2, half, lanes), jnp.bfloat16) for lanes in (part, part - TILE)]
        + [jax.ShapeDtypeStruct((layers, 2, half, hidden), jnp.float32)]
        + [store] * 4,
        scratch_shapes=[
            pltpu.VMEM((2, 2, 4, half, hidden), jnp.bfloat16),
            pltpu.VMEM((2, 2 * part, half), jnp.bfloat16),
            pltpu.VMEM((4, half, part), jnp.bfloat16),
            pltpu.VMEM((2, 2 * part, half), jnp.float32),
            pltpu.VMEM((4, 2, rows, hidden), jnp.float32),
            pltpu.VMEM((2, rows, hidden), jnp.bfloat16),
            dma((layers, 2)),
            dma((layers, 2)),
            dma((layers, 2)),
            dma((layers, 2)),
            dma((layers, 2)),
            dma((layers, 2)),
            dma((layers,)),
            dma((layers, 2)),
            dma((layers, 2)),
            dma((layers,)),
            dma((4, part // TILE)),
            dma((4, part // TILE)),
            dma((part // TILE, 2)),
            dma((part // TILE, 2)),
            dma((part // TILE,)),
            dma((part // TILE,)),
            dma((2,)),
            dma((2,)),
            dma((4, 2)),
            dma((2,)),
            dma((4,)),
            dma((2, 4)),
            dma((part // TILE,)),
        ],
        compiler_params=pltpu.CompilerParams(vmem_limit_bytes=60 * 1024 * 1024, has_side_effects=True),
        name="stack",
    )(lr, w_up, g_up, w_down, g_down, xt)


def place_kernel(gen_ref, raw, *refs, first, last, final):
    nu, nd, buf, sem_in, sem_out = refs[-5:]
    layers = raw.shape[0]
    is_gen = gen_ref[0] == 1
    slots = buf.shape[0]

    def out(place, l, k):
        return pltpu.make_async_copy(buf.at[place], (nu, nd)[k].at[l], sem_out.at[place])

    if final:

        @pl.when(is_gen)
        def _():
            zeros = [(i % slots, i // 2, i % 2) for i in range(2 * layers)]
            buf[...] = jnp.zeros_like(buf)
            for i, at in enumerate(zeros):
                if i >= slots:
                    out(*zeros[i - slots]).wait()
                out(*at).start()
            for at in zeros[-slots:]:
                out(*at).wait()

    @pl.when(jnp.logical_not(is_gen))
    def _():
        items = [(i % slots, first + i // 2, i % 2) for i in range(2 * (last - first))]
        lead = slots // 2

        def load(place, l, k):
            return pltpu.make_async_copy(raw.at[l, k], buf.at[place], sem_in.at[place])

        for at in items[:lead]:
            load(*at).start()
        for i, at in enumerate(items):
            if i + lead < len(items):
                if i >= lead:
                    out(*items[i - lead]).wait()
                load(*items[i + lead]).start()
            load(*at).wait()
            out(*at).start()
        for at in items[-min(slots, len(items)) :]:
            out(*at).wait()


def place_update(gen, raw, prev, first, last):
    layers, _, half, hidden = raw.shape
    shape = jax.ShapeDtypeStruct((layers, half, hidden), jnp.float32)
    prev = list(prev or ())
    nbytes = (last - first) * half * hidden * 4 * 4
    any_spec = pl.BlockSpec(memory_space=pl.ANY)
    return pl.pallas_call(
        functools.partial(place_kernel, first=first, last=last, final=last == layers),
        in_specs=[pl.BlockSpec(memory_space=pltpu.SMEM)] + [any_spec] * (1 + len(prev)),
        out_specs=[any_spec] * 2,
        out_shape=[shape] * 2,
        scratch_shapes=[
            pltpu.VMEM((PLACE_SLOTS, half, hidden), jnp.float32),
            pltpu.SemaphoreType.DMA((PLACE_SLOTS,)),
            pltpu.SemaphoreType.DMA((PLACE_SLOTS,)),
        ],
        input_output_aliases={2: 0, 3: 1} if prev else {},
        compiler_params=pltpu.CompilerParams(vmem_limit_bytes=40 * 1024 * 1024),
        cost_estimate=pl.CostEstimate(flops=nbytes * 30, bytes_accessed=nbytes, transcendentals=0),
        name="place",
    )(gen, raw, *prev)


def solution(mesh):
    reps = mesh.shape["rep"]
    axes = ("side", "rep")

    def at(side, rep):
        return side * reps + rep

    pairs = [(t, c) for t in range(2) for c in range(2)]
    up_spec = P("side", None, "rep", None)
    down_spec = P("side", None, None, "rep")
    act_spec = P("side", "rep", None)

    def device_step(w_up, w_down, g_up, g_down, learn_rate, prompts, prompt_lens):
        side = lax.axis_index("side")
        core = lax.axis_index("rep")
        is_gen = side >= 2
        t = lax.rem(side, 2)
        tokens, half = prompts.shape[1], prompts.shape[2]
        part = tokens // 4
        lr = learn_rate.reshape(1)

        w_up, g_up = w_up[0], g_up[0]
        w_down, g_down = jnp.swapaxes(w_down[0], 1, 2), jnp.swapaxes(g_down[0], 1, 2)
        xt = jnp.swapaxes(prompts[0], 0, 1)
        *outs, mine, theirs, raw = mlp_stack(lr, w_up, g_up, w_down, g_down, xt)[:5]
        gen = is_gen.astype(jnp.int32).reshape(1)
        layers = raw.shape[0]
        placed = place_update(gen, raw, None, 0, EARLY)
        outs = lax.optimization_barrier((*outs, *placed))[:2]

        back = []
        for dt in range(2):
            perm = [(at(a, b), at(2 + (a ^ dt), 1 - b)) for a, b in pairs]
            back.append(lax.ppermute(outs[dt], axes, perm))

        new_up, new_down = place_update(gen, raw, placed, EARLY, layers)

        pieces = []
        for tj in range(2):
            handed = jnp.concatenate([theirs[tj], jnp.where(t == tj, back[0], back[1])], axis=1)
            pieces += [jnp.where(core == cj, mine[tj], handed) for cj in range(2)]
        y = jnp.concatenate(pieces, axis=1)
        keep = (jnp.arange(tokens)[None, :] < prompt_lens[0]) & is_gen
        y = jnp.swapaxes(jnp.where(keep, y, jnp.zeros_like(y)), 0, 1)
        return new_up[None], jnp.swapaxes(new_down, 1, 2)[None], y[None]

    return jax.shard_map(
        device_step,
        mesh=mesh,
        in_specs=(up_spec, down_spec, up_spec, down_spec, P(), act_spec, P("rep")),
        out_specs=(up_spec, down_spec, act_spec),
        check_vma=False,
    )
```

```python
import functools

import jax
import jax.numpy as jnp
from jax import lax
from jax.experimental import pallas as pl
from jax.experimental.pallas import tpu as pltpu
from jax.sharding import PartitionSpec as P


HAND = 10
DIRECT = 2
MIXED = DIRECT - 1
TILE = 512
ARRIVE = 3
UPDATE_SPLIT = 2
PLACE_SLOTS = 8
EARLY = 2
LAST = (((1,), (1,)), ((), ()))
GELU_A = 0.7978845608
GELU_B = 0.7978845608 * 0.044715
MESH = pl.DeviceIdType.MESH


def gelu(z):
    t = jnp.tanh(z * (GELU_A + GELU_B * (z * z)))
    h = 0.5 * z
    return h + h * t


def flip(index, by):
    return 1 - index if by else index


def stack_kernel(lr_ref, wu, gu, wd, gd, xt, *refs):
    outs, (yin, zin, raw), (own, recv, pown, pfwd), refs = refs[:2], refs[2:5], refs[5:9], refs[9:]
    wv, act, xr, psum, fbuf, obuf = refs[:6]
    s_own, r_own, s_main, r_main, s_fwd, r_fwd, s_a, s_b, r_b, s_c, s_x, r_x, s_h, r_h, s_y, r_y, s_z, r_z = refs[6:24]
    sem_in, sem_out, sem_raw, sem_ld, sem_y = refs[24:]
    side, core = lax.axis_index("side"), lax.axis_index("rep")
    t = lax.rem(side, 2)
    layers, half, hidden = wu.shape
    rows = half // UPDATE_SPLIT
    part = xt.shape[1] // 4
    spread = part // TILE
    tiles = 2 * spread

    def remote(src, dst, send, recv_sem, to):
        return pltpu.make_async_remote_copy(
            src_ref=src, dst_ref=dst, send_sem=send, recv_sem=recv_sem, device_id=to, device_id_type=MESH
        )

    def x_send(dt, dc, h):
        slot = 2 * dt + dc
        to = (flip(t, dt), flip(core, dc))
        lane = pl.multiple_of((2 * to[0] + to[1]) * part + h * TILE, 128)
        dst = xr.at[slot, :, pl.ds(h * TILE, TILE)]
        return remote(xt.at[:, pl.ds(lane, TILE)], dst, s_x.at[slot, h], r_x.at[slot, h], to)

    def x_recv(dt, tile):
        slot, h = 2 * dt + tile // spread, lax.rem(tile, spread)
        dst = xr.at[slot, :, pl.ds(pl.multiple_of(h * TILE, 128), TILE)]
        return remote(dst, dst, s_x.at[slot, h], r_x.at[slot, h], (t, core))

    def own_copy(l, k):
        return remote(own.at[l, k], pown.at[l, k], s_own.at[l, k], r_own.at[l, k], (side, 1 - core))

    def fwd_copy(l, k):
        return remote(recv.at[l, k], pfwd.at[l, k], s_fwd.at[l, k], r_fwd.at[l, k], (side, 1 - core))

    def main_copy(l, k):
        return remote(own.at[l, k], recv.at[l, k], s_main.at[l, k], r_main.at[l, k], (1 - t, core))

    def a_copy(l, k):
        sent = s_main.at[l, 1] if k else s_a.at[l]
        return remote(own.at[l, k], own.at[l, k], sent, r_main.at[l, k], (2 + t, core))

    def b_copy(l, k):
        return remote(own.at[l, k], recv.at[l, k], s_b.at[l, k], r_b.at[l, k], (3 - t, core))

    def c_copy(l):
        return remote(recv.at[l, 1], recv.at[l, 1], s_c.at[l], r_main.at[l, 1], (t, core))

    first_rows, last_rows = pl.ds(0, rows), pl.ds(rows, half - rows)

    def direct_half():
        src, dst = own.at[MIXED, 1, first_rows], recv.at[MIXED, 1, first_rows]
        return remote(src, dst, s_main.at[MIXED, 1], r_main.at[MIXED, 1], (1 - t, core))

    def a_half():
        ref = own.at[MIXED, 1, last_rows]
        return remote(ref, ref, s_a.at[MIXED], r_main.at[MIXED, 1], (2 + t, core))

    def b_half():
        src, dst = own.at[MIXED, 1, last_rows], recv.at[MIXED, 1, last_rows]
        return remote(src, dst, s_b.at[MIXED, 1], r_b.at[MIXED, 1], (3 - t, core))

    def c_half():
        ref = recv.at[MIXED, 1, last_rows]
        return remote(ref, ref, s_c.at[MIXED], r_b.at[MIXED, 0], (t, core))

    def h_copy(tile, s):
        rows_of = act.at[s, pl.ds(pl.multiple_of(tile * TILE, TILE), TILE)]
        return remote(rows_of, rows_of, s_h.at[tile, s], r_h.at[tile, s], (2 + t, core))

    def y_copy(tile):
        lanes = pl.ds(pl.multiple_of(tile * TILE, TILE), TILE)
        return remote(xr.at[2, :, lanes], yin.at[t, :, lanes], s_y.at[tile], r_y.at[tile], (3 - t, core))

    def y_arrival(tile):
        lanes = pl.ds(pl.multiple_of(tile * TILE, TILE), TILE)
        dst = yin.at[1 - t, :, lanes]
        return remote(dst, dst, s_y.at[tile], r_y.at[tile], (3 - t, core))

    def y_keep(tile):
        lanes = pl.ds(pl.multiple_of(tile * TILE, TILE), TILE)
        return pltpu.make_async_copy(xr.at[0, :, lanes], yin.at[t, :, lanes], sem_y.at[tile])

    def z_copy(dt):
        lanes = pl.ds(0, part - TILE)
        src, dst = xr.at[2 * dt + 1, :, lanes], zin.at[t]
        return remote(src, dst, s_z.at[dt], r_z.at[t], (2 + flip(t, dt), 1 - core))

    def z_arrival(tj):
        return remote(zin.at[tj], zin.at[tj], s_z.at[0], r_z.at[tj], (tj, 1 - core))

    twist = lax.rem(core + t, 2)

    def fetch(l, k, place):
        src = (own, pown, recv, pfwd)[place]
        slot = lax.rem(l, 2)
        return pltpu.make_async_copy(src.at[l, k], wv.at[slot, k, place], sem_ld.at[k, place])

    def fetched(l, q):
        for k in range(2):
            for place in (2 * q, 2 * q + 1):
                fetch(l, k, place).wait()

    def half_tile(l, q, tile):
        slot = lax.rem(l, 2)
        span = pl.ds(pl.multiple_of(tile * TILE, TILE), TILE)
        x0, x1 = act[0, span, :], act[1, span, :]
        z = jnp.dot(x0, wv[slot, 0, 2 * q], preferred_element_type=jnp.float32)
        z = z + jnp.dot(x1, wv[slot, 0, 2 * q + 1], preferred_element_type=jnp.float32)
        u = gelu(z).astype(jnp.bfloat16)
        p0 = lax.dot_general(u, wv[slot, 1, 2 * q], LAST, preferred_element_type=jnp.float32)
        p1 = lax.dot_general(u, wv[slot, 1, 2 * q + 1], LAST, preferred_element_type=jnp.float32)
        return span, (x0, x1), (p0, p1)

    def x_out(tile):
        def turn(step, carry):
            lane = pl.multiple_of(lax.rem(tile, spread) * TILE + step * 128, 128)
            row = pl.multiple_of(tile * TILE + step * 128, 128)
            for dt in range(2):
                slot = 2 * dt + tile // spread
                xr[slot, :, pl.ds(lane, 128)] = jnp.transpose(act[flip(twist, dt), pl.ds(row, 128), :])
            return carry

        lax.fori_loop(0, TILE // 128, turn, 0)

    def first_half(l, tile):
        span, _, sums = half_tile(l, 0, tile)
        for s in range(2):
            psum[s, span, :] = sums[s]

    def second_half(l, tile):
        span, xs, sums = half_tile(l, 1, tile)
        for s in range(2):
            total = psum[s, span, :] + sums[s]
            act[s, span, :] = (xs[s].astype(jnp.float32) + total).astype(jnp.bfloat16)

    @pl.when(side >= 2)
    def _():
        for dc in range(2):
            for h in range(spread):
                for dt in range(2):
                    x_send(dt, dc, h).start()

        def relay(l):
            b_copy(l, 1).wait_recv()
            c_copy(l).start()

            @pl.when(l >= HAND)
            def _():
                fwd_copy(l, 1).start()

        def hop(l, carry):
            a_copy(l, 1).wait_recv()
            b_copy(l, 1).start()

            @pl.when(l >= HAND)
            def _():
                own_copy(l, 1).start()

            @pl.when(l == DIRECT)
            def _():
                b_half().wait_recv()
                c_half().start()

            @pl.when(l > DIRECT)
            def _():
                relay(l - 1)

            return carry

        a_half().wait_recv()
        b_half().start()
        lax.fori_loop(DIRECT, layers, hop, 0)
        relay(layers - 1)
        for l in range(HAND, layers):
            a_copy(l, 0).wait_recv()
            b_copy(l, 0).start()
            own_copy(l, 0).start()
        for l in range(HAND, layers):
            b_copy(l, 0).wait_recv()
            fwd_copy(l, 0).start()
        for l in range(HAND, layers):
            for k in range(2):
                own_copy(l, k).wait_recv()
                fwd_copy(l, k).wait_recv()
                for place in range(4):
                    fetch(l, k, place).start()
            fetched(l, 0)
            fetched(l, 1)

        def finish(tile, carry):
            for s in range(2):
                h_copy(tile, s).wait_recv()

            def layer(l, carry):
                first_half(l, tile)
                second_half(l, tile)
                return carry

            lax.fori_loop(HAND, layers, layer, 0)
            x_out(tile)
            y_copy(tile).start()
            y_keep(tile).start()
            return carry

        lax.fori_loop(0, spread, finish, 0)

        def drain(l, carry):
            b_copy(l, 1).wait_send()
            c_copy(l).wait_send()
            return carry

        lax.fori_loop(DIRECT, layers, drain, 0)
        b_half().wait_send()
        c_half().wait_send()
        for l in range(HAND, layers):
            b_copy(l, 0).wait_send()
            for k in range(2):
                own_copy(l, k).wait_send()
                fwd_copy(l, k).wait_send()
        for tile in range(spread):
            y_keep(tile).wait()
            y_copy(tile).wait_send()
            y_arrival(tile).wait_recv()
        for tj in range(2):
            z_arrival(tj).wait_recv()
        for dc in range(2):
            for h in range(spread):
                for dt in range(2):
                    x_send(dt, dc, h).wait_send()

    @pl.when(side < 2)
    def _():
        lr = lr_ref[0]

        def loads(l, unit):
            k, h = unit // 2, unit % 2
            w, g = ((wu, gu), (wd, gd))[k]
            span = pl.ds(h * rows, rows)
            return (
                pltpu.make_async_copy(w.at[l, span], fbuf.at[unit, 0], sem_in.at[unit, 0]),
                pltpu.make_async_copy(g.at[l, span], fbuf.at[unit, 1], sem_in.at[unit, 1]),
            )

        def raw_store(l, unit):
            k, h = unit // 2, unit % 2
            return pltpu.make_async_copy(fbuf.at[unit, 0], raw.at[l, k, pl.ds(h * rows, rows)], sem_raw.at[unit])

        def store(l, unit):
            k, h = unit // 2, unit % 2
            return pltpu.make_async_copy(obuf.at[h], own.at[l, k, pl.ds(h * rows, rows)], sem_out.at[h])

        def send(l, k):
            own_copy(l, k).start()
            if k == 0:
                main_copy(l, 0).start()
                return

            @pl.when(l < MIXED)
            def _():
                main_copy(l, 1).start()

            @pl.when(l == MIXED)
            def _():
                direct_half().start()
                a_half().start()

            @pl.when(l >= DIRECT)
            def _():
                a_copy(l, 1).start()

        for unit in range(2):
            for copy in loads(0, unit):
                copy.start()

        def update(l, carry):
            for unit in range(4):
                h = unit % 2
                ahead = (unit + 2) % 4
                if unit < 2:

                    @pl.when(l > 0)
                    def _():
                        raw_store(l - 1, ahead).wait()

                    for copy in loads(l, ahead):
                        copy.start()
                else:

                    @pl.when(l + 1 < layers)
                    def _():
                        raw_store(l, ahead).wait()
                        for copy in loads(l + 1, ahead):
                            copy.start()

                for copy in loads(l, unit):
                    copy.wait()
                if unit >= 2:
                    store(l, unit - 2).wait()
                    if h == 1:
                        send(l, 0)
                else:

                    @pl.when(l > 0)
                    def _():
                        store(l - 1, unit + 2).wait()
                        if h == 1:
                            send(l - 1, 1)

                new = fbuf[unit, 0] - lr * fbuf[unit, 1]
                fbuf[unit, 0] = new
                obuf[h] = new.astype(jnp.bfloat16)
                raw_store(l, unit).start()
                store(l, unit).start()
            return carry

        lax.fori_loop(0, layers, update, 0)
        store(layers - 1, 2).wait()
        store(layers - 1, 3).wait()
        for unit in range(4):
            raw_store(layers - 1, unit).wait()
        send(layers - 1, 1)
        for l in range(HAND, layers):
            a_copy(l, 0).start()

        def x_in(tile):
            for dt in range(2):
                x_recv(dt, tile).wait_recv()

            def turn(step, carry):
                lane = pl.multiple_of(lax.rem(tile, spread) * TILE + step * 128, 128)
                row = pl.multiple_of(tile * TILE + step * 128, 128)
                for dt in range(2):
                    slot = 2 * dt + tile // spread
                    act[flip(twist, dt), pl.ds(row, 128), :] = jnp.transpose(xr[slot, :, pl.ds(lane, 128)])
                return carry

            lax.fori_loop(0, TILE // 128, turn, 0)

        def fetch_own(l):
            for k in range(2):
                fetch(l, k, 0).start()
                own_copy(l, k).wait_recv()
                fetch(l, k, 1).start()

        def fetch_recv(l):
            for k in (1, 0):
                if k == 0:
                    main_copy(l, k).wait_recv()
                else:

                    @pl.when(l == MIXED)
                    def _():
                        direct_half().wait_recv()
                        c_half().wait_recv()

                    @pl.when(l != MIXED)
                    def _():
                        main_copy(l, 1).wait_recv()

                fwd_copy(l, k).start()
                fetch(l, k, 2).start()

        def fetch_fwd(l):
            for k in (1, 0):
                fwd_copy(l, k).wait_recv()
                fetch(l, k, 3).start()

        fetch_own(0)

        def layer(l, carry):
            fetched(l, 0)

            @pl.when(l + 1 < layers)
            def _():
                fetch_own(l + 1)

            def first(tile, carry):
                @pl.when(l == 0)
                def _():
                    x_in(tile)

                @pl.when(tile == ARRIVE)
                def _():
                    fetch_recv(l)

                first_half(l, tile)
                return carry

            start = spread * (l // HAND)
            lax.fori_loop(start, tiles, first, 0)
            fetch_fwd(l)
            fetched(l, 1)

            def second(tile, carry):
                @pl.when((l == HAND - 1) & (tile >= 1) & (tile <= spread))
                def _():
                    for s in range(2):
                        h_copy(tile - 1, s).start()

                second_half(l, tile)

                @pl.when(l == layers - 1)
                def _():
                    x_out(tile)

                @pl.when((l == layers - 1) & (tile == tiles - 2))
                def _():
                    for dt in range(2):
                        z_copy(dt).start()

                return carry

            lax.fori_loop(start, tiles, second, 0)
            return carry

        lax.fori_loop(0, layers, layer, 0)

        lanes = pl.ds(part - TILE, TILE)
        y_copies = [pltpu.make_async_copy(xr.at[2 * dt + 1, :, lanes], outs[dt], sem_y.at[dt]) for dt in range(2)]
        for copy in y_copies:
            copy.start()
        for copy in y_copies:
            copy.wait()

        def drain(l, carry):
            for k in range(2):
                own_copy(l, k).wait_send()
                fwd_copy(l, k).wait_send()
            main_copy(l, 0).wait_send()

            @pl.when(l == MIXED)
            def _():
                direct_half().wait_send()
                a_half().wait_send()

            @pl.when(l != MIXED)
            def _():
                main_copy(l, 1).wait_send()

            return carry

        lax.fori_loop(0, layers, drain, 0)
        for l in range(HAND, layers):
            a_copy(l, 0).wait_send()
        for tile in range(spread):
            for s in range(2):
                h_copy(tile, s).wait_send()
        for dt in range(2):
            z_copy(dt).wait_send()


def mlp_stack(lr, w_up, g_up, w_down, g_down, xt):
    layers, half, hidden = w_up.shape
    part = xt.shape[1] // 4
    rows = half // UPDATE_SPLIT
    dma = pltpu.SemaphoreType.DMA
    any_spec = pl.BlockSpec(memory_space=pl.ANY)
    store = jax.ShapeDtypeStruct((layers, 2, half, hidden), jnp.bfloat16)
    return pl.pallas_call(
        stack_kernel,
        in_specs=[pl.BlockSpec(memory_space=pltpu.SMEM)] + [any_spec] * 5,
        out_specs=[any_spec] * 9,
        out_shape=[jax.ShapeDtypeStruct((half, TILE), jnp.bfloat16)] * 2
        + [jax.ShapeDtypeStruct((2, half, lanes), jnp.bfloat16) for lanes in (part, part - TILE)]
        + [jax.ShapeDtypeStruct((layers, 2, half, hidden), jnp.float32)]
        + [store] * 4,
        scratch_shapes=[
            pltpu.VMEM((2, 2, 4, half, hidden), jnp.bfloat16),
            pltpu.VMEM((2, 2 * part, half), jnp.bfloat16),
            pltpu.VMEM((4, half, part), jnp.bfloat16),
            pltpu.VMEM((2, 2 * part, half), jnp.float32),
            pltpu.VMEM((4, 2, rows, hidden), jnp.float32),
            pltpu.VMEM((2, rows, hidden), jnp.bfloat16),
            dma((layers, 2)),
            dma((layers, 2)),
            dma((layers, 2)),
            dma((layers, 2)),
            dma((layers, 2)),
            dma((layers, 2)),
            dma((layers,)),
            dma((layers, 2)),
            dma((layers, 2)),
            dma((layers,)),
            dma((4, part // TILE)),
            dma((4, part // TILE)),
            dma((part // TILE, 2)),
            dma((part // TILE, 2)),
            dma((part // TILE,)),
            dma((part // TILE,)),
            dma((2,)),
            dma((2,)),
            dma((4, 2)),
            dma((2,)),
            dma((4,)),
            dma((2, 4)),
            dma((part // TILE,)),
        ],
        compiler_params=pltpu.CompilerParams(vmem_limit_bytes=60 * 1024 * 1024, has_side_effects=True),
        name="stack",
    )(lr, w_up, g_up, w_down, g_down, xt)


def place_kernel(gen_ref, raw, *refs, first, last, final):
    nu, nd, buf, sem_in, sem_out = refs[-5:]
    layers = raw.shape[0]
    is_gen = gen_ref[0] == 1
    slots = buf.shape[0]

    def out(place, l, k):
        return pltpu.make_async_copy(buf.at[place], (nu, nd)[k].at[l], sem_out.at[place])

    if final:

        @pl.when(is_gen)
        def _():
            zeros = [(i % slots, i // 2, i % 2) for i in range(2 * layers)]
            buf[...] = jnp.zeros_like(buf)
            for i, at in enumerate(zeros):
                if i >= slots:
                    out(*zeros[i - slots]).wait()
                out(*at).start()
            for at in zeros[-slots:]:
                out(*at).wait()

    @pl.when(jnp.logical_not(is_gen))
    def _():
        items = [(i % slots, first + i // 2, i % 2) for i in range(2 * (last - first))]
        lead = slots // 2

        def load(place, l, k):
            return pltpu.make_async_copy(raw.at[l, k], buf.at[place], sem_in.at[place])

        for at in items[:lead]:
            load(*at).start()
        for i, at in enumerate(items):
            if i + lead < len(items):
                if i >= lead:
                    out(*items[i - lead]).wait()
                load(*items[i + lead]).start()
            load(*at).wait()
            out(*at).start()
        for at in items[-min(slots, len(items)) :]:
            out(*at).wait()


def place_update(gen, raw, prev, first, last):
    layers, _, half, hidden = raw.shape
    shape = jax.ShapeDtypeStruct((layers, half, hidden), jnp.float32)
    prev = list(prev or ())
    nbytes = (last - first) * half * hidden * 4 * 4
    any_spec = pl.BlockSpec(memory_space=pl.ANY)
    return pl.pallas_call(
        functools.partial(place_kernel, first=first, last=last, final=last == layers),
        in_specs=[pl.BlockSpec(memory_space=pltpu.SMEM)] + [any_spec] * (1 + len(prev)),
        out_specs=[any_spec] * 2,
        out_shape=[shape] * 2,
        scratch_shapes=[
            pltpu.VMEM((PLACE_SLOTS, half, hidden), jnp.float32),
            pltpu.SemaphoreType.DMA((PLACE_SLOTS,)),
            pltpu.SemaphoreType.DMA((PLACE_SLOTS,)),
        ],
        input_output_aliases={2: 0, 3: 1} if prev else {},
        compiler_params=pltpu.CompilerParams(vmem_limit_bytes=40 * 1024 * 1024),
        cost_estimate=pl.CostEstimate(flops=nbytes * 30, bytes_accessed=nbytes, transcendentals=0),
        name="place",
    )(gen, raw, *prev)


def solution(mesh):
    reps = mesh.shape["rep"]
    axes = ("side", "rep")

    def at(side, rep):
        return side * reps + rep

    pairs = [(t, c) for t in range(2) for c in range(2)]
    up_spec = P("side", None, "rep", None)
    down_spec = P("side", None, None, "rep")
    act_spec = P("side", "rep", None)

    def device_step(w_up, w_down, g_up, g_down, learn_rate, prompts, prompt_lens):
        side = lax.axis_index("side")
        core = lax.axis_index("rep")
        is_gen = side >= 2
        t = lax.rem(side, 2)
        tokens, half = prompts.shape[1], prompts.shape[2]
        part = tokens // 4
        lr = learn_rate.reshape(1)

        w_up, g_up = w_up[0], g_up[0]
        w_down, g_down = jnp.swapaxes(w_down[0], 1, 2), jnp.swapaxes(g_down[0], 1, 2)
        xt = jnp.swapaxes(prompts[0], 0, 1)
        *outs, mine, theirs, raw = mlp_stack(lr, w_up, g_up, w_down, g_down, xt)[:5]
        gen = is_gen.astype(jnp.int32).reshape(1)
        layers = raw.shape[0]
        placed = place_update(gen, raw, None, 0, EARLY)
        outs = lax.optimization_barrier((*outs, *placed))[:2]

        back = []
        for dt in range(2):
            perm = [(at(a, b), at(2 + (a ^ dt), 1 - b)) for a, b in pairs]
            back.append(lax.ppermute(outs[dt], axes, perm))

        new_up, new_down = place_update(gen, raw, placed, EARLY, layers)

        pieces = []
        for tj in range(2):
            handed = jnp.concatenate([theirs[tj], jnp.where(t == tj, back[0], back[1])], axis=1)
            pieces += [jnp.where(core == cj, mine[tj], handed) for cj in range(2)]
        y = jnp.concatenate(pieces, axis=1)
        keep = (jnp.arange(tokens)[None, :] < prompt_lens[0]) & is_gen
        y = jnp.swapaxes(jnp.where(keep, y, jnp.zeros_like(y)), 0, 1)
        return new_up[None], jnp.swapaxes(new_down, 1, 2)[None], y[None]

    return jax.shard_map(
        device_step,
        mesh=mesh,
        in_specs=(up_spec, down_spec, up_spec, down_spec, P(), act_spec, P("rep")),
        out_specs=(up_spec, down_spec, act_spec),
        check_vma=False,
    )
```

```python
import functools

import jax
import jax.numpy as jnp
from jax import lax
from jax.experimental import pallas as pl
from jax.experimental.pallas import tpu as pltpu
from jax.sharding import PartitionSpec as P


HAND = 10
DIRECT = 2
TILE = 512
ARRIVE = 3
UPDATE_SPLIT = 2
SENT = 256
PLACE_SLOTS = 8
EARLY = 2
LAST = (((1,), (1,)), ((), ()))
GELU_A = 0.7978845608
GELU_B = 0.7978845608 * 0.044715
MESH = pl.DeviceIdType.MESH


def gelu(z):
    t = jnp.tanh(z * (GELU_A + GELU_B * (z * z)))
    h = 0.5 * z
    return h + h * t


def flip(index, by):
    return 1 - index if by else index


def stack_kernel(lr_ref, wu, gu, wd, gd, xt, *refs):
    outs, (yin, zin, raw), (own, recv, pown, pfwd), refs = refs[:2], refs[2:5], refs[5:9], refs[9:]
    wv, act, xr, psum, fbuf, obuf = refs[:6]
    s_own, r_own, s_main, r_main, s_fwd, r_fwd, s_a, s_b, r_b, s_c, s_x, r_x, s_h, r_h, s_y, r_y, s_z, r_z = refs[6:24]
    sem_in, sem_out, sem_raw, sem_ld, sem_y = refs[24:]
    side, core = lax.axis_index("side"), lax.axis_index("rep")
    t = lax.rem(side, 2)
    layers, half, hidden = wu.shape
    rows = half // UPDATE_SPLIT
    part = xt.shape[1] // 4
    spread = part // TILE
    tiles = 2 * spread

    def remote(src, dst, send, recv_sem, to):
        return pltpu.make_async_remote_copy(
            src_ref=src, dst_ref=dst, send_sem=send, recv_sem=recv_sem, device_id=to, device_id_type=MESH
        )

    def x_send(dt, dc, h):
        slot = 2 * dt + dc
        to = (flip(t, dt), flip(core, dc))
        lane = pl.multiple_of((2 * to[0] + to[1]) * part + h * TILE, 128)
        dst = xr.at[slot, :, pl.ds(h * TILE, TILE)]
        return remote(xt.at[:, pl.ds(lane, TILE)], dst, s_x.at[slot, h], r_x.at[slot, h], to)

    def x_recv(dt, tile):
        slot, h = 2 * dt + tile // spread, lax.rem(tile, spread)
        dst = xr.at[slot, :, pl.ds(pl.multiple_of(h * TILE, 128), TILE)]
        return remote(dst, dst, s_x.at[slot, h], r_x.at[slot, h], (t, core))

    def own_copy(l, k):
        return remote(own.at[l, k], pown.at[l, k], s_own.at[l, k], r_own.at[l, k], (side, 1 - core))

    def fwd_copy(l, k):
        return remote(recv.at[l, k], pfwd.at[l, k], s_fwd.at[l, k], r_fwd.at[l, k], (side, 1 - core))

    def main_copy(l, k):
        return remote(own.at[l, k], recv.at[l, k], s_main.at[l, k], r_main.at[l, k], (1 - t, core))

    def a_copy(l, k):
        sent = s_main.at[l, 1] if k else s_a.at[l]
        return remote(own.at[l, k], own.at[l, k], sent, r_main.at[l, k], (2 + t, core))

    def b_copy(l, k):
        return remote(own.at[l, k], recv.at[l, k], s_b.at[l, k], r_b.at[l, k], (3 - t, core))

    def c_copy(l):
        return remote(recv.at[l, 1], recv.at[l, 1], s_c.at[l], r_main.at[l, 1], (t, core))

    def h_copy(tile, s):
        rows_of = act.at[s, pl.ds(pl.multiple_of(tile * TILE, TILE), TILE)]
        return remote(rows_of, rows_of, s_h.at[tile, s], r_h.at[tile, s], (2 + t, core))

    def y_copy(tile):
        lanes = pl.ds(pl.multiple_of(tile * TILE, TILE), TILE)
        return remote(xr.at[2, :, lanes], yin.at[t, :, lanes], s_y.at[tile], r_y.at[tile], (3 - t, core))

    def y_arrival(tile):
        lanes = pl.ds(pl.multiple_of(tile * TILE, TILE), TILE)
        dst = yin.at[1 - t, :, lanes]
        return remote(dst, dst, s_y.at[tile], r_y.at[tile], (3 - t, core))

    def y_keep(tile):
        lanes = pl.ds(pl.multiple_of(tile * TILE, TILE), TILE)
        return pltpu.make_async_copy(xr.at[0, :, lanes], yin.at[t, :, lanes], sem_y.at[tile])

    def z_copy(dt):
        lanes = pl.ds(0, SENT)
        src, dst = xr.at[2 * dt + 1, :, lanes], zin.at[t]
        return remote(src, dst, s_z.at[dt], r_z.at[t], (2 + flip(t, dt), 1 - core))

    def z_arrival(tj):
        return remote(zin.at[tj], zin.at[tj], s_z.at[0], r_z.at[tj], (tj, 1 - core))

    twist = lax.rem(core + t, 2)

    def fetch(l, k, place):
        src = (own, pown, recv, pfwd)[place]
        slot = lax.rem(l, 2)
        return pltpu.make_async_copy(src.at[l, k], wv.at[slot, k, place], sem_ld.at[k, place])

    def fetched(l, q):
        for k in range(2):
            for place in (2 * q, 2 * q + 1):
                fetch(l, k, place).wait()

    def half_tile(l, q, tile):
        slot = lax.rem(l, 2)
        span = pl.ds(pl.multiple_of(tile * TILE, TILE), TILE)
        x0, x1 = act[0, span, :], act[1, span, :]
        z = jnp.dot(x0, wv[slot, 0, 2 * q], preferred_element_type=jnp.float32)
        z = z + jnp.dot(x1, wv[slot, 0, 2 * q + 1], preferred_element_type=jnp.float32)
        u = gelu(z).astype(jnp.bfloat16)
        p0 = lax.dot_general(u, wv[slot, 1, 2 * q], LAST, preferred_element_type=jnp.float32)
        p1 = lax.dot_general(u, wv[slot, 1, 2 * q + 1], LAST, preferred_element_type=jnp.float32)
        return span, (x0, x1), (p0, p1)

    def x_out(tile):
        def turn(step, carry):
            lane = pl.multiple_of(lax.rem(tile, spread) * TILE + step * 128, 128)
            row = pl.multiple_of(tile * TILE + step * 128, 128)
            for dt in range(2):
                slot = 2 * dt + tile // spread
                xr[slot, :, pl.ds(lane, 128)] = jnp.transpose(act[flip(twist, dt), pl.ds(row, 128), :])
            return carry

        lax.fori_loop(0, TILE // 128, turn, 0)

    def first_half(l, tile):
        span, _, sums = half_tile(l, 0, tile)
        for s in range(2):
            psum[s, span, :] = sums[s]

    def second_half(l, tile):
        span, xs, sums = half_tile(l, 1, tile)
        for s in range(2):
            total = psum[s, span, :] + sums[s]
            act[s, span, :] = (xs[s].astype(jnp.float32) + total).astype(jnp.bfloat16)

    @pl.when(side >= 2)
    def _():
        for dc in range(2):
            for h in range(spread):
                for dt in range(2):
                    x_send(dt, dc, h).start()

        def relay(l):
            b_copy(l, 1).wait_recv()
            c_copy(l).start()

            @pl.when(l >= HAND)
            def _():
                fwd_copy(l, 1).start()

        def hop(l, carry):
            a_copy(l, 1).wait_recv()
            b_copy(l, 1).start()

            @pl.when(l >= HAND)
            def _():
                own_copy(l, 1).start()

            @pl.when(l > DIRECT)
            def _():
                relay(l - 1)

            return carry

        lax.fori_loop(DIRECT, layers, hop, 0)
        relay(layers - 1)
        for l in range(HAND, layers):
            a_copy(l, 0).wait_recv()
            b_copy(l, 0).start()
            own_copy(l, 0).start()
        for l in range(HAND, layers):
            b_copy(l, 0).wait_recv()
            fwd_copy(l, 0).start()
        def fetch_all(l):
            for k in (1, 0):
                own_copy(l, k).wait_recv()
                fwd_copy(l, k).wait_recv()
                for place in range(4):
                    fetch(l, k, place).start()
            fetched(l, 0)
            fetched(l, 1)

        taken = layers - HAND

        def finish(index, carry):
            l, tile = HAND + index % taken, index // taken

            @pl.when(index < taken)
            def _():
                fetch_all(l)

            @pl.when(l == HAND)
            def _():
                for s in range(2):
                    h_copy(tile, s).wait_recv()

            first_half(l, tile)
            second_half(l, tile)

            @pl.when(l == layers - 1)
            def _():
                x_out(tile)
                y_copy(tile).start()
                y_keep(tile).start()

            return carry

        lax.fori_loop(0, taken * spread, finish, 0)

        def drain(l, carry):
            b_copy(l, 1).wait_send()
            c_copy(l).wait_send()
            return carry

        lax.fori_loop(DIRECT, layers, drain, 0)
        for l in range(HAND, layers):
            b_copy(l, 0).wait_send()
            for k in range(2):
                own_copy(l, k).wait_send()
                fwd_copy(l, k).wait_send()
        for tile in range(spread):
            y_keep(tile).wait()
            y_copy(tile).wait_send()
            y_arrival(tile).wait_recv()
        for tj in range(2):
            z_arrival(tj).wait_recv()
        for dc in range(2):
            for h in range(spread):
                for dt in range(2):
                    x_send(dt, dc, h).wait_send()

    @pl.when(side < 2)
    def _():
        lr = lr_ref[0]

        def loads(l, unit):
            k, h = unit // 2, unit % 2
            w, g = ((wu, gu), (wd, gd))[k]
            span = pl.ds(h * rows, rows)
            return (
                pltpu.make_async_copy(w.at[l, span], fbuf.at[unit, 0], sem_in.at[unit, 0]),
                pltpu.make_async_copy(g.at[l, span], fbuf.at[unit, 1], sem_in.at[unit, 1]),
            )

        def raw_store(l, unit):
            k, h = unit // 2, unit % 2
            return pltpu.make_async_copy(fbuf.at[unit, 0], raw.at[l, k, pl.ds(h * rows, rows)], sem_raw.at[unit])

        def store(l, unit):
            k, h = unit // 2, unit % 2
            return pltpu.make_async_copy(obuf.at[h], own.at[l, k, pl.ds(h * rows, rows)], sem_out.at[h])

        def send(l, k):
            own_copy(l, k).start()
            if k == 0:
                main_copy(l, 0).start()
                return

            @pl.when(l < DIRECT)
            def _():
                main_copy(l, 1).start()

            @pl.when(l >= DIRECT)
            def _():
                a_copy(l, 1).start()

        for unit in range(2):
            for copy in loads(0, unit):
                copy.start()

        def update(l, carry):
            for unit in range(4):
                h = unit % 2
                ahead = (unit + 2) % 4
                if unit < 2:

                    @pl.when(l > 0)
                    def _():
                        raw_store(l - 1, ahead).wait()

                    for copy in loads(l, ahead):
                        copy.start()
                else:

                    @pl.when(l + 1 < layers)
                    def _():
                        raw_store(l, ahead).wait()
                        for copy in loads(l + 1, ahead):
                            copy.start()

                for copy in loads(l, unit):
                    copy.wait()
                if unit >= 2:
                    store(l, unit - 2).wait()
                    if h == 1:
                        send(l, 0)
                else:

                    @pl.when(l > 0)
                    def _():
                        store(l - 1, unit + 2).wait()
                        if h == 1:
                            send(l - 1, 1)

                new = fbuf[unit, 0] - lr * fbuf[unit, 1]
                fbuf[unit, 0] = new
                obuf[h] = new.astype(jnp.bfloat16)
                raw_store(l, unit).start()
                store(l, unit).start()
            return carry

        lax.fori_loop(0, layers, update, 0)
        store(layers - 1, 2).wait()
        store(layers - 1, 3).wait()
        for unit in range(4):
            raw_store(layers - 1, unit).wait()
        send(layers - 1, 1)
        for l in range(HAND, layers):
            a_copy(l, 0).start()

        def x_in(tile):
            for dt in range(2):
                x_recv(dt, tile).wait_recv()

            def turn(step, carry):
                lane = pl.multiple_of(lax.rem(tile, spread) * TILE + step * 128, 128)
                row = pl.multiple_of(tile * TILE + step * 128, 128)
                for dt in range(2):
                    slot = 2 * dt + tile // spread
                    act[flip(twist, dt), pl.ds(row, 128), :] = jnp.transpose(xr[slot, :, pl.ds(lane, 128)])
                return carry

            lax.fori_loop(0, TILE // 128, turn, 0)

        def fetch_own(l):
            for k in range(2):
                fetch(l, k, 0).start()
                own_copy(l, k).wait_recv()
                fetch(l, k, 1).start()

        def fetch_recv(l):
            for k in (1, 0):
                main_copy(l, k).wait_recv()
                fwd_copy(l, k).start()
                fetch(l, k, 2).start()

        def fetch_fwd(l):
            for k in (1, 0):
                fwd_copy(l, k).wait_recv()
                fetch(l, k, 3).start()

        fetch_own(0)

        def layer(l, carry):
            fetched(l, 0)

            @pl.when(l + 1 < layers)
            def _():
                fetch_own(l + 1)

            def first(tile, carry):
                @pl.when(l == 0)
                def _():
                    x_in(tile)

                @pl.when(tile == ARRIVE)
                def _():
                    fetch_recv(l)

                first_half(l, tile)
                return carry

            start = spread * (l // HAND)
            lax.fori_loop(start, tiles, first, 0)
            fetch_fwd(l)
            fetched(l, 1)

            def second(tile, carry):
                @pl.when((l == HAND - 1) & (tile >= 1) & (tile <= spread))
                def _():
                    for s in range(2):
                        h_copy(tile - 1, s).start()

                second_half(l, tile)

                @pl.when(l == layers - 1)
                def _():
                    x_out(tile)

                @pl.when((l == layers - 1) & (tile == tiles - 2))
                def _():
                    for dt in range(2):
                        z_copy(dt).start()

                return carry

            lax.fori_loop(start, tiles, second, 0)
            return carry

        lax.fori_loop(0, layers, layer, 0)

        lanes = pl.ds(SENT, part - SENT)
        y_copies = [pltpu.make_async_copy(xr.at[2 * dt + 1, :, lanes], outs[dt], sem_y.at[dt]) for dt in range(2)]
        for copy in y_copies:
            copy.start()
        for copy in y_copies:
            copy.wait()

        def drain(l, carry):
            for k in range(2):
                own_copy(l, k).wait_send()
                main_copy(l, k).wait_send()
                fwd_copy(l, k).wait_send()
            return carry

        lax.fori_loop(0, layers, drain, 0)
        for l in range(HAND, layers):
            a_copy(l, 0).wait_send()
        for tile in range(spread):
            for s in range(2):
                h_copy(tile, s).wait_send()
        for dt in range(2):
            z_copy(dt).wait_send()


def mlp_stack(lr, w_up, g_up, w_down, g_down, xt):
    layers, half, hidden = w_up.shape
    part = xt.shape[1] // 4
    rows = half // UPDATE_SPLIT
    dma = pltpu.SemaphoreType.DMA
    any_spec = pl.BlockSpec(memory_space=pl.ANY)
    store = jax.ShapeDtypeStruct((layers, 2, half, hidden), jnp.bfloat16)
    return pl.pallas_call(
        stack_kernel,
        in_specs=[pl.BlockSpec(memory_space=pltpu.SMEM)] + [any_spec] * 5,
        out_specs=[any_spec] * 9,
        out_shape=[jax.ShapeDtypeStruct((half, part - SENT), jnp.bfloat16)] * 2
        + [jax.ShapeDtypeStruct((2, half, lanes), jnp.bfloat16) for lanes in (part, SENT)]
        + [jax.ShapeDtypeStruct((layers, 2, half, hidden), jnp.float32)]
        + [store] * 4,
        scratch_shapes=[
            pltpu.VMEM((2, 2, 4, half, hidden), jnp.bfloat16),
            pltpu.VMEM((2, 2 * part, half), jnp.bfloat16),
            pltpu.VMEM((4, half, part), jnp.bfloat16),
            pltpu.VMEM((2, 2 * part, half), jnp.float32),
            pltpu.VMEM((4, 2, rows, hidden), jnp.float32),
            pltpu.VMEM((2, rows, hidden), jnp.bfloat16),
            dma((layers, 2)),
            dma((layers, 2)),
            dma((layers, 2)),
            dma((layers, 2)),
            dma((layers, 2)),
            dma((layers, 2)),
            dma((layers,)),
            dma((layers, 2)),
            dma((layers, 2)),
            dma((layers,)),
            dma((4, part // TILE)),
            dma((4, part // TILE)),
            dma((part // TILE, 2)),
            dma((part // TILE, 2)),
            dma((part // TILE,)),
            dma((part // TILE,)),
            dma((2,)),
            dma((2,)),
            dma((4, 2)),
            dma((2,)),
            dma((4,)),
            dma((2, 4)),
            dma((part // TILE,)),
        ],
        compiler_params=pltpu.CompilerParams(vmem_limit_bytes=60 * 1024 * 1024, has_side_effects=True),
        name="stack",
    )(lr, w_up, g_up, w_down, g_down, xt)


def place_kernel(gen_ref, raw, *refs, first, last, final):
    nu, nd, buf, sem_in, sem_out = refs[-5:]
    layers = raw.shape[0]
    is_gen = gen_ref[0] == 1
    slots = buf.shape[0]

    def out(place, l, k):
        return pltpu.make_async_copy(buf.at[place], (nu, nd)[k].at[l], sem_out.at[place])

    if final:

        @pl.when(is_gen)
        def _():
            zeros = [(i % slots, i // 2, i % 2) for i in range(2 * layers)]
            buf[...] = jnp.zeros_like(buf)
            for i, at in enumerate(zeros):
                if i >= slots:
                    out(*zeros[i - slots]).wait()
                out(*at).start()
            for at in zeros[-slots:]:
                out(*at).wait()

    @pl.when(jnp.logical_not(is_gen))
    def _():
        items = [(i % slots, first + i // 2, i % 2) for i in range(2 * (last - first))]
        lead = slots // 2

        def load(place, l, k):
            return pltpu.make_async_copy(raw.at[l, k], buf.at[place], sem_in.at[place])

        for at in items[:lead]:
            load(*at).start()
        for i, at in enumerate(items):
            if i + lead < len(items):
                if i >= lead:
                    out(*items[i - lead]).wait()
                load(*items[i + lead]).start()
            load(*at).wait()
            out(*at).start()
        for at in items[-min(slots, len(items)) :]:
            out(*at).wait()


def place_update(gen, raw, prev, first, last):
    layers, _, half, hidden = raw.shape
    shape = jax.ShapeDtypeStruct((layers, half, hidden), jnp.float32)
    prev = list(prev or ())
    nbytes = (last - first) * half * hidden * 4 * 4
    any_spec = pl.BlockSpec(memory_space=pl.ANY)
    return pl.pallas_call(
        functools.partial(place_kernel, first=first, last=last, final=last == layers),
        in_specs=[pl.BlockSpec(memory_space=pltpu.SMEM)] + [any_spec] * (1 + len(prev)),
        out_specs=[any_spec] * 2,
        out_shape=[shape] * 2,
        scratch_shapes=[
            pltpu.VMEM((PLACE_SLOTS, half, hidden), jnp.float32),
            pltpu.SemaphoreType.DMA((PLACE_SLOTS,)),
            pltpu.SemaphoreType.DMA((PLACE_SLOTS,)),
        ],
        input_output_aliases={2: 0, 3: 1} if prev else {},
        compiler_params=pltpu.CompilerParams(vmem_limit_bytes=40 * 1024 * 1024),
        cost_estimate=pl.CostEstimate(flops=nbytes * 30, bytes_accessed=nbytes, transcendentals=0),
        name="place",
    )(gen, raw, *prev)


def solution(mesh):
    reps = mesh.shape["rep"]
    axes = ("side", "rep")

    def at(side, rep):
        return side * reps + rep

    pairs = [(t, c) for t in range(2) for c in range(2)]
    up_spec = P("side", None, "rep", None)
    down_spec = P("side", None, None, "rep")
    act_spec = P("side", "rep", None)

    def device_step(w_up, w_down, g_up, g_down, learn_rate, prompts, prompt_lens):
        side = lax.axis_index("side")
        core = lax.axis_index("rep")
        is_gen = side >= 2
        t = lax.rem(side, 2)
        tokens, half = prompts.shape[1], prompts.shape[2]
        part = tokens // 4
        lr = learn_rate.reshape(1)

        w_up, g_up = w_up[0], g_up[0]
        w_down, g_down = jnp.swapaxes(w_down[0], 1, 2), jnp.swapaxes(g_down[0], 1, 2)
        xt = jnp.swapaxes(prompts[0], 0, 1)
        *outs, mine, theirs, raw = mlp_stack(lr, w_up, g_up, w_down, g_down, xt)[:5]
        gen = is_gen.astype(jnp.int32).reshape(1)
        layers = raw.shape[0]
        placed = place_update(gen, raw, None, 0, EARLY)
        outs = lax.optimization_barrier((*outs, *placed))[:2]

        back = []
        for dt in range(2):
            perm = [(at(a, b), at(2 + (a ^ dt), 1 - b)) for a, b in pairs]
            back.append(lax.ppermute(outs[dt], axes, perm))

        new_up, new_down = place_update(gen, raw, placed, EARLY, layers)

        pieces = []
        for tj in range(2):
            handed = jnp.concatenate([theirs[tj], jnp.where(t == tj, back[0], back[1])], axis=1)
            pieces += [jnp.where(core == cj, mine[tj], handed) for cj in range(2)]
        y = jnp.concatenate(pieces, axis=1)
        keep = (jnp.arange(tokens)[None, :] < prompt_lens[0]) & is_gen
        y = jnp.swapaxes(jnp.where(keep, y, jnp.zeros_like(y)), 0, 1)
        return new_up[None], jnp.swapaxes(new_down, 1, 2)[None], y[None]

    return jax.shard_map(
        device_step,
        mesh=mesh,
        in_specs=(up_spec, down_spec, up_spec, down_spec, P(), act_spec, P("rep")),
        out_specs=(up_spec, down_spec, act_spec),
        check_vma=False,
    )
```
